32 devices in a mesh: tp: 32 (over z, y, x, core).
Axes of the slice: x: 2, y: 2, z: 4, core: 2. Of those that a mesh axis runs over, the one named last changes fastest.
Arguments:
- x_input: bfloat16 [1, 3072, 4096], P(None, 'tp')
- w_query: bfloat16 [4096, 4096], P(None, 'tp')
- w_key: bfloat16 [4096, 4096], P(None, 'tp')
- w_value: bfloat16 [4096, 4096], P(None, 'tp')
- w_out: bfloat16 [4096, 4096], P('tp')
- g_query: bfloat16 [4096], P('tp')
- g_key: bfloat16 [4096], P('tp')
- g_attn: bfloat16 [4096], replicated
- grad_y: bfloat16 [1, 3072, 4096], P(None, 'tp')
Outputs:
- output 1: bfloat16 [1, 3072, 4096], P(None, 'tp')
- output 2: bfloat16 [1, 3072, 4096], P(None, 'tp')
- output 3: bfloat16 [4096, 4096], P(None, 'tp')
- output 4: bfloat16 [4096, 4096], P(None, 'tp')
- output 5: bfloat16 [4096, 4096], P(None, 'tp')
- output 6: bfloat16 [4096, 4096], P('tp')
- output 7: bfloat16 [4096], P('tp')
- output 8: bfloat16 [4096], P('tp')
- output 9: bfloat16 [4096], replicated
All inputs are finite; a program needn't handle non-finite values.
Results may differ from the reference program's by a relative error of at most 0.0172326.
Values are sent between devices in bfloat16 or wider.
A program may use at most 1 GiB of HBM per device.

```python
import jax
import jax.numpy as jnp
from jax import lax

BATCH_SIZE = 1
SEQ_LEN = 3072
MODEL_DIM = 4096
NUM_HEADS = 32
HEAD_DIM = 128
ROPE_THETA = 500000
NORM_EPS = 1e-6


def setup_inputs(seed: int = 0) -> dict:
    rng_keys = jax.random.split(jax.random.key(seed), 12)
    fan_scale = MODEL_DIM ** -0.5
    act_shape = (BATCH_SIZE, SEQ_LEN, MODEL_DIM)
    mat_shape = (MODEL_DIM, MODEL_DIM)
    head_q = jnp.exp(jax.random.uniform(rng_keys[0], (NUM_HEADS,), jnp.float32, jnp.log(0.3), jnp.log(3.0)))
    head_k = jnp.exp(jax.random.uniform(rng_keys[1], (NUM_HEADS,), jnp.float32, jnp.log(0.3), jnp.log(3.0)))
    col_q = jnp.repeat(head_q, HEAD_DIM)[None, :]
    col_k = jnp.repeat(head_k, HEAD_DIM)[None, :]
    x_input = jax.random.normal(rng_keys[2], act_shape, jnp.float32)
    w_query = jax.random.normal(rng_keys[3], mat_shape, jnp.float32) * fan_scale * col_q
    w_key = jax.random.normal(rng_keys[4], mat_shape, jnp.float32) * fan_scale * col_k
    w_value = jax.random.normal(rng_keys[5], mat_shape, jnp.float32) * fan_scale
    w_out = jax.random.normal(rng_keys[6], mat_shape, jnp.float32) * fan_scale
    g_query = jax.random.uniform(rng_keys[7], (MODEL_DIM,), jnp.float32, 0.5, 1.5)
    g_key = jax.random.uniform(rng_keys[8], (MODEL_DIM,), jnp.float32, 0.5, 1.5)
    g_attn = jax.random.uniform(rng_keys[9], (MODEL_DIM,), jnp.float32, 0.5, 1.5)
    grad_y = jax.random.normal(rng_keys[10], act_shape, jnp.float32)
    return {'x_input': x_input.astype(jnp.bfloat16), 'w_query': w_query.astype(jnp.bfloat16), 'w_key': w_key.astype(jnp.bfloat16), 'w_value': w_value.astype(jnp.bfloat16), 'w_out': w_out.astype(jnp.bfloat16), 'g_query': g_query.astype(jnp.bfloat16), 'g_key': g_key.astype(jnp.bfloat16), 'g_attn': g_attn.astype(jnp.bfloat16), 'grad_y': grad_y.astype(jnp.bfloat16)}


def rope_tables():
    half_dim = HEAD_DIM // 2
    inv_freq = 1.0 / (ROPE_THETA ** (jnp.arange(half_dim, dtype=jnp.float32) / half_dim))
    angles = jnp.arange(SEQ_LEN, dtype=jnp.float32)[:, None] * inv_freq[None, :]
    return jnp.cos(angles)[:, None, :], jnp.sin(angles)[:, None, :]


def rotate(values, cos_t, sin_t):
    lower_half, upper_half = jnp.split(values, 2, axis=-1)
    return jnp.concatenate([lower_half * cos_t - upper_half * sin_t, upper_half * cos_t + lower_half * sin_t], axis=-1)


def whole_norm(values, gain):
    inv_rms = lax.rsqrt(jnp.mean(values * values, axis=-1, keepdims=True) + NORM_EPS)
    return values * inv_rms * gain.astype(jnp.float32)


def head_attention(operands):
    q_head, k_head, v_head = operands
    scores = jnp.einsum('bqd,bkd->bqk', q_head.astype(jnp.float32), k_head.astype(jnp.float32)) * (HEAD_DIM ** -0.5)
    causal = jnp.arange(SEQ_LEN)[:, None] >= jnp.arange(SEQ_LEN)[None, :]
    attn_probs = jax.nn.softmax(jnp.where(causal[None], scores, -1e30), axis=-1)
    head_out = jnp.einsum('bqk,bkd->bqd', attn_probs.astype(jnp.bfloat16).astype(jnp.float32), v_head.astype(jnp.float32))
    return head_out.astype(jnp.bfloat16)


def block_forward(x_input, w_query, w_key, w_value, w_out, g_query, g_key, g_attn):
    x_rows = x_input.reshape(BATCH_SIZE * SEQ_LEN, MODEL_DIM)
    head_shape = (BATCH_SIZE, SEQ_LEN, NUM_HEADS, HEAD_DIM)
    cos_t, sin_t = rope_tables()
    q_raw = jnp.dot(x_rows, w_query, preferred_element_type=jnp.float32)
    k_raw = jnp.dot(x_rows, w_key, preferred_element_type=jnp.float32)
    v_proj = jnp.dot(x_rows, w_value, preferred_element_type=jnp.float32).astype(jnp.bfloat16)
    q_rot = rotate(whole_norm(q_raw, g_query).reshape(head_shape), cos_t, sin_t).astype(jnp.bfloat16)
    k_rot = rotate(whole_norm(k_raw, g_key).reshape(head_shape), cos_t, sin_t).astype(jnp.bfloat16)
    v_heads = v_proj.reshape(head_shape)
    per_head = lax.map(jax.checkpoint(head_attention), (jnp.moveaxis(q_rot, 2, 0), jnp.moveaxis(k_rot, 2, 0), jnp.moveaxis(v_heads, 2, 0)))
    attn_rows = jnp.moveaxis(per_head, 0, 2).reshape(BATCH_SIZE * SEQ_LEN, MODEL_DIM)
    attn_sum = jnp.dot(attn_rows, w_out, preferred_element_type=jnp.float32)
    post_rms = lax.rsqrt(jnp.mean(attn_sum * attn_sum, axis=-1, keepdims=True) + NORM_EPS)
    y_rows = x_rows.astype(jnp.float32) + attn_sum * post_rms * g_attn.astype(jnp.float32)
    return y_rows.astype(jnp.bfloat16).reshape(BATCH_SIZE, SEQ_LEN, MODEL_DIM)


def reference(x_input, w_query, w_key, w_value, w_out, g_query, g_key, g_attn, grad_y):
    y_out, pullback = jax.vjp(block_forward, x_input, w_query, w_key, w_value, w_out, g_query, g_key, g_attn)
    grad_x, grad_wq, grad_wk, grad_wv, grad_wo, grad_gq, grad_gk, grad_ga = pullback(grad_y)
    return (y_out, grad_x, grad_wq, grad_wk, grad_wv, grad_wo, grad_gq, grad_gk, grad_ga)
```

```python
import functools

import jax
import jax.numpy as jnp
from jax import lax
from jax.experimental import pallas as pl
from jax.experimental.pallas import tpu as pltpu
from jax.sharding import PartitionSpec as P

HEAD_SIZE = 128
ROPE_THETA = 500000.0
NORM_EPS = 1e-6
LOG2E = 1.4426950408889634
ATTN_SCALE = HEAD_SIZE ** -0.5
MESH = pl.DeviceIdType.MESH
VMEM = pl.BlockSpec(memory_space=pltpu.VMEM)
BLOCK = 512


def rope_tables(seq_len):
    half_dim = HEAD_SIZE // 2
    inv_freq = 1.0 / (ROPE_THETA ** (jnp.arange(half_dim, dtype=jnp.float32) / half_dim))
    angles = jnp.arange(seq_len, dtype=jnp.float32)[:, None] * inv_freq[None, :]
    return jnp.cos(angles), jnp.sin(angles)


def rotate(values, cos_t, sin_t):
    lower_half, upper_half = jnp.split(values, 2, axis=-1)
    return jnp.concatenate([lower_half * cos_t - upper_half * sin_t, upper_half * cos_t + lower_half * sin_t], axis=-1)


def rotate_back(values, cos_t, sin_t):
    lower_half, upper_half = jnp.split(values, 2, axis=-1)
    return jnp.concatenate([lower_half * cos_t + upper_half * sin_t, upper_half * cos_t - lower_half * sin_t], axis=-1)


def column_of(me):
    z, c, core = me // 8, lax.rem(me // 2, 4), lax.rem(me, 2)
    return z * 2 + core, c


def column_peer(me, k):
    m, c = column_of(me)
    m2 = lax.rem(m + k, 8)
    return (m2 // 2) * 8 + c * 2 + lax.rem(m2, 2)


def plane_peer(me, k):
    return (me // 8) * 8 + lax.rem(lax.rem(me, 8) + k, 8)


def ring_peer(me, k):
    c = lax.rem(lax.rem(me // 2, 4) + k, 4)
    return (me // 8) * 8 + c * 2 + lax.rem(me, 2)


def line_peer(me, k):
    return lax.rem(me // 8 + k, 4) * 8 + lax.rem(me, 8)


def entry_barrier(me, peer_of, count):
    barrier = pltpu.get_barrier_semaphore()
    for k in range(1, count):
        pl.semaphore_signal(barrier, inc=1, device_id=(peer_of(me, k),), device_id_type=MESH)
    pl.semaphore_wait(barrier, count - 1)


def exchange_kernel(peer_of, count, source, target, x_ref, out_ref, send_sem, recv_sem):
    me = lax.axis_index('tp')
    entry_barrier(me, peer_of, count)
    copies = []
    for k in range(1, count):
        peer = peer_of(me, k)
        copy = pltpu.make_async_remote_copy(
            src_ref=source(x_ref, peer), dst_ref=target(out_ref, me),
            send_sem=send_sem.at[k], recv_sem=recv_sem.at[k], device_id=(peer,), device_id_type=MESH)
        copy.start()
        copies.append(copy)
    target(out_ref, me)[...] = source(x_ref, me)[...]
    for copy in copies:
        copy.wait()


def exchange(x, out_shape, peer_of, count, source, target, collective_id):
    return pl.pallas_call(
        functools.partial(exchange_kernel, peer_of, count, source, target),
        out_shape=jax.ShapeDtypeStruct(out_shape, x.dtype),
        in_specs=[VMEM], out_specs=VMEM,
        scratch_shapes=[pltpu.SemaphoreType.DMA((count,)), pltpu.SemaphoreType.DMA((count,))],
        compiler_params=pltpu.CompilerParams(collective_id=collective_id, has_side_effects=True, vmem_limit_bytes=24 << 20),
    )(x)


def reduce_kernel(peer_of, count, rank_of, x_ref, out_ref, parts, send_sem, recv_sem):
    me = lax.axis_index('tp')
    entry_barrier(me, peer_of, count)
    copies = []
    for k in range(1, count):
        peer = peer_of(me, k)
        copy = pltpu.make_async_remote_copy(
            src_ref=x_ref.at[rank_of(peer)], dst_ref=parts.at[k - 1],
            send_sem=send_sem.at[k], recv_sem=recv_sem.at[k], device_id=(peer,), device_id_type=MESH)
        copy.start()
        copies.append(copy)
    mine = rank_of(me)
    for copy in copies:
        copy.wait()

    def add(i, carry):
        rows = pl.ds(pl.multiple_of(i * 8, 8), 8)
        total = x_ref[mine, rows, :]
        for k in range(count - 1):
            total = total + parts[k, rows, :]
        out_ref[rows, :] = total
        return carry

    lax.fori_loop(0, out_ref.shape[0] // 8, add, 0)


def reduce_scatter(x, peer_of, rank_of, collective_id):
    count, rows, cols = x.shape
    return pl.pallas_call(
        functools.partial(reduce_kernel, peer_of, count, rank_of),
        out_shape=jax.ShapeDtypeStruct((rows, cols), x.dtype),
        in_specs=[VMEM], out_specs=VMEM,
        scratch_shapes=[pltpu.VMEM((count - 1, rows, cols), x.dtype),
                        pltpu.SemaphoreType.DMA((count,)), pltpu.SemaphoreType.DMA((count,))],
        compiler_params=pltpu.CompilerParams(collective_id=collective_id, has_side_effects=True, vmem_limit_bytes=32 << 20),
    )(x)


def all_sum_kernel(x_ref, out_ref, plane, middle, line, send_sem, recv_sem):
    me = lax.axis_index('tp')
    barrier = pltpu.get_barrier_semaphore()
    for k in range(1, 8):
        pl.semaphore_signal(barrier, inc=1, device_id=(plane_peer(me, k),), device_id_type=MESH)
    for k in range(1, 4):
        pl.semaphore_signal(barrier, inc=1, device_id=(line_peer(me, k),), device_id_type=MESH)
    pl.semaphore_wait(barrier, 10)
    mine = lax.rem(me, 8)
    copies = []
    for k in range(1, 8):
        copy = pltpu.make_async_remote_copy(
            src_ref=x_ref, dst_ref=plane.at[mine], send_sem=send_sem.at[k], recv_sem=recv_sem.at[k],
            device_id=(plane_peer(me, k),), device_id_type=MESH)
        copy.start()
        copies.append(copy)
    plane[mine] = x_ref[...]
    for copy in copies:
        copy.wait()
    total = plane[0]
    for k in range(1, 8):
        total = total + plane[k]
    middle[...] = total
    z = me // 8
    line[z] = total
    copies = []
    for k in range(1, 4):
        copy = pltpu.make_async_remote_copy(
            src_ref=middle, dst_ref=line.at[z], send_sem=send_sem.at[7 + k], recv_sem=recv_sem.at[7 + k],
            device_id=(line_peer(me, k),), device_id_type=MESH)
        copy.start()
        copies.append(copy)
    for copy in copies:
        copy.wait()
    out_ref[...] = (line[0] + line[1]) + (line[2] + line[3])


def all_sum(x, collective_id):
    return pl.pallas_call(
        all_sum_kernel,
        out_shape=jax.ShapeDtypeStruct(x.shape, x.dtype),
        in_specs=[VMEM], out_specs=VMEM,
        scratch_shapes=[pltpu.VMEM((8,) + x.shape, x.dtype), pltpu.VMEM(x.shape, x.dtype), pltpu.VMEM((4,) + x.shape, x.dtype),
                        pltpu.SemaphoreType.DMA((11,)), pltpu.SemaphoreType.DMA((11,))],
        compiler_params=pltpu.CompilerParams(collective_id=collective_id, has_side_effects=True, vmem_limit_bytes=8 << 20),
    )(x)


def greet(peers):
    barrier = pltpu.get_barrier_semaphore()
    for peer in peers:
        pl.semaphore_signal(barrier, inc=1, device_id=(peer,), device_id_type=MESH)
    pl.semaphore_wait(barrier, len(peers))


def send(src, dst, sems, slot, peer):
    copy = pltpu.make_async_remote_copy(
        src_ref=src, dst_ref=dst, send_sem=sems[0].at[slot], recv_sem=sems[1].at[slot], device_id=(peer,), device_id_type=MESH)
    copy.start()
    return copy


def semaphores(count):
    return [pltpu.SemaphoreType.DMA((count,)), pltpu.SemaphoreType.DMA((count,))]


def spread_kernel(x_ref, ring_ref, near_ref, *sems):
    me = lax.axis_index('tp')
    greet([ring_peer(me, k) for k in range(1, 4)] + [line_peer(me, 1), line_peer(me, 3)])
    mine = lax.rem(me // 2, 4)
    copies = [send(x_ref, ring_ref.at[mine], sems, k, ring_peer(me, k)) for k in range(1, 4)]
    copies += [send(x_ref, near_ref.at[0], sems, 4, line_peer(me, 1)), send(x_ref, near_ref.at[1], sems, 5, line_peer(me, 3))]
    ring_ref[mine] = x_ref[...]
    for copy in copies:
        copy.wait()


def spread(x, collective_id):
    return pl.pallas_call(
        spread_kernel,
        out_shape=(jax.ShapeDtypeStruct((4,) + x.shape, x.dtype), jax.ShapeDtypeStruct((2,) + x.shape, x.dtype)),
        in_specs=[VMEM], out_specs=(VMEM, VMEM), scratch_shapes=semaphores(6),
        compiler_params=pltpu.CompilerParams(collective_id=collective_id, has_side_effects=True, vmem_limit_bytes=24 << 20),
    )(x)


def plane_kernel(width, x_ref, d_ref, out_ref, far_ref, *sems):
    me = lax.axis_index('tp')
    greet([plane_peer(me, k) for k in range(1, 8)] + [line_peer(me, 2)])
    mine = lax.rem(me, 8)
    columns = pl.ds(pl.multiple_of(mine * width, width), width)
    copies = [send(d_ref, far_ref, sems, 0, line_peer(me, 2))]
    for k in range(1, 8):
        peer = plane_peer(me, k)
        copies.append(send(x_ref.at[:, lax.rem(peer, 8)], out_ref.at[:, :, columns], sems, k, peer))
    out_ref[:, :, columns] = x_ref[:, mine]
    for copy in copies:
        copy.wait()


def plane_exchange(x, d, collective_id):
    width = x.shape[-1]
    return pl.pallas_call(
        functools.partial(plane_kernel, width),
        out_shape=(jax.ShapeDtypeStruct((4, x.shape[2], 8 * width), x.dtype), jax.ShapeDtypeStruct(d.shape, d.dtype)),
        in_specs=[VMEM, VMEM], out_specs=(VMEM, VMEM), scratch_shapes=semaphores(8),
        compiler_params=pltpu.CompilerParams(collective_id=collective_id, has_side_effects=True, vmem_limit_bytes=24 << 20),
    )(x, d)


TILE = 512


def final_kernel(dx_ref, ring_ref, near_ref, far_ref, dw_ref, o_ref, x_ref, sum_ref, gw_ref, gwo_ref,
                 parts, full, x_buf, x_sem, local_sem, *sems):
    me = lax.axis_index('tp')
    z, c, core = me // 8, lax.rem(me // 2, 4), lax.rem(me, 2)
    partner = me + 1 - 2 * core
    greet([line_peer(me, k) for k in range(1, 4)] + [ring_peer(me, k) for k in range(1, 4)] + [partner])
    sums = [send(dx_ref.at[line_peer(me, k) // 8], parts.at[k - 1], sems, k - 1, line_peer(me, k)) for k in (2, 1, 3)]
    planes = [lax.rem(z + 3, 4), lax.rem(z + 1, 4), lax.rem(z + 2, 4)]
    lines = [near_ref.at[0], near_ref.at[1], far_ref]

    def slot(plane, column):
        return plane * 8 + column * 2 + core

    rounds, shared, local = [], [], []
    for r in range(3):
        for k in range(1, 4):
            rounds.append(send(lines[r], full.at[slot(planes[r], c)], sems, 3 + r * 3 + k - 1, ring_peer(me, k)))
    for r in range(3):
        shared.append(send(lines[r], full.at[slot(planes[r], c)], sems, 12 + r, partner))
        local.append(pltpu.make_async_copy(lines[r], full.at[slot(planes[r], c)], local_sem.at[r]))
    for j in range(4):
        shared.append(send(ring_ref.at[j], full.at[slot(z, j)], sems, 15 + j, partner))
        local.append(pltpu.make_async_copy(ring_ref.at[j], full.at[slot(z, j)], local_sem.at[3 + j]))
    for copy in local:
        copy.start()

    tiles = x_ref.shape[1] // TILE

    def columns(j):
        return pl.ds(pl.multiple_of(j * TILE, TILE), TILE)

    def fetch(j, b):
        return pltpu.make_async_copy(x_ref.at[:, columns(j)], x_buf.at[b], x_sem.at[b])

    fetch(0, 0).start()

    def weights(j, carry):
        b = lax.rem(j, 2)

        @pl.when(j + 1 < tiles)
        def _():
            fetch(j + 1, 1 - b).start()

        fetch(j, b).wait()
        gw_ref[:, columns(j)] = nn(dw_ref[...], x_buf[b]).astype(gw_ref.dtype)
        return carry

    lax.fori_loop(0, tiles, weights, 0)
    for r in range(3):
        for k in range(1, 4):
            rounds[r * 3 + k - 1].wait()
            block = full.at[slot(planes[r], lax.rem(c + 4 - k, 4))]
            shared.append(send(block, block, sems, 19 + r * 3 + k - 1, partner))
    for copy in sums:
        copy.wait()

    def add(i, carry):
        rows = pl.ds(pl.multiple_of(i * 8, 8), 8)
        sum_ref[rows, :] = (dx_ref[z, rows, :] + parts[0, rows, :]) + (parts[1, rows, :] + parts[2, rows, :])
        return carry

    lax.fori_loop(0, sum_ref.shape[0] // 8, add, 0)
    for copy in local:
        copy.wait()
    for copy in shared:
        copy.wait()

    def out_weights(j, carry):
        d = full[:, :, columns(j)]
        gwo_ref[:, columns(j)] = nn(o_ref[...], d.reshape(o_ref.shape[1], TILE)).astype(gwo_ref.dtype)
        return carry

    lax.fori_loop(0, tiles, out_weights, 0)


def final(dx_part, d_ring, d_near, d_far, dw_rows, o_rows, x_full, collective_id):
    count, rows, model_dim = dx_part.shape
    seq_len = x_full.shape[0]
    anywhere = pl.BlockSpec(memory_space=pl.ANY)
    return pl.pallas_call(
        final_kernel,
        out_shape=(jax.ShapeDtypeStruct((rows, model_dim), jnp.float32),
                   jax.ShapeDtypeStruct((dw_rows.shape[0], model_dim), jnp.bfloat16),
                   jax.ShapeDtypeStruct((o_rows.shape[0], model_dim), jnp.bfloat16)),
        in_specs=[VMEM, anywhere, anywhere, anywhere, VMEM, VMEM, anywhere], out_specs=(VMEM, VMEM, VMEM),
        scratch_shapes=[pltpu.VMEM((count - 1, rows, model_dim), jnp.float32),
                        pltpu.VMEM((seq_len // rows, rows, model_dim), jnp.bfloat16),
                        pltpu.VMEM((2, seq_len, TILE), jnp.bfloat16),
                        pltpu.SemaphoreType.DMA((2,)), pltpu.SemaphoreType.DMA((7,))] + semaphores(28),
        compiler_params=pltpu.CompilerParams(collective_id=collective_id, has_side_effects=True, vmem_limit_bytes=60 << 20),
    )(dx_part, d_ring, d_near, d_far, dw_rows, o_rows, x_full)


def nt(a, b):
    return lax.dot_general(a, b, (((1,), (1,)), ((), ())), preferred_element_type=jnp.float32)


def tn(a, b):
    return lax.dot_general(a, b, (((0,), (0,)), ((), ())), preferred_element_type=jnp.float32)


def nn(a, b):
    return lax.dot_general(a, b, (((1,), (0,)), ((), ())), preferred_element_type=jnp.float32)


def fold_rows(values, op):
    return op(values.reshape(values.shape[0] // 8, 8, values.shape[1]), axis=0)


def block_rows(j):
    return pl.ds(pl.multiple_of(j * BLOCK, BLOCK), BLOCK)


def diagonal_mask():
    keys = lax.broadcasted_iota(jnp.int32, (BLOCK, BLOCK), 0)
    queries = lax.broadcasted_iota(jnp.int32, (BLOCK, BLOCK), 1)
    return keys <= queries


def attention_kernel(q_ref, k_ref, v_ref, o_ref, max_ref, inv_ref, s_scr, acc_scr):
    i = pl.program_id(0)
    q_blk = q_ref[...]

    def score(j, top):
        s = nt(k_ref[block_rows(j), :], q_blk) * (ATTN_SCALE * LOG2E)
        s_scr[block_rows(j), :] = s
        return jnp.maximum(top, fold_rows(s, jnp.max))

    s = jnp.where(diagonal_mask(), nt(k_ref[block_rows(i), :], q_blk) * (ATTN_SCALE * LOG2E), -1e30)
    s_scr[block_rows(i), :] = s
    top = lax.fori_loop(0, i, score, fold_rows(s, jnp.max))
    top = jnp.max(top, axis=0, keepdims=True)

    def weigh(j, total):
        p = jnp.exp2(s_scr[block_rows(j), :] - top)
        s_scr[block_rows(j), :] = p
        return total + fold_rows(p, jnp.sum)

    total = lax.fori_loop(0, i + 1, weigh, jnp.zeros((8, BLOCK), jnp.float32))
    inv = 1.0 / jnp.sum(total, axis=0, keepdims=True)
    max_ref[...] = top
    inv_ref[...] = inv
    acc_scr[...] = jnp.zeros_like(acc_scr)

    def gather(j, carry):
        p = (s_scr[block_rows(j), :] * inv).astype(jnp.bfloat16)
        acc_scr[...] += tn(v_ref[block_rows(j), :], p)
        return carry

    lax.fori_loop(0, i + 1, gather, 0)
    o_ref[...] = acc_scr[...].T.astype(jnp.bfloat16)


def attention(q, k, v):
    seq_len = q.shape[0]
    steps = seq_len // BLOCK
    rows = pl.BlockSpec((BLOCK, HEAD_SIZE), lambda i: (i, 0))
    whole = pl.BlockSpec((seq_len, HEAD_SIZE), lambda i: (0, 0))
    line = pl.BlockSpec((1, BLOCK), lambda i: (0, i))
    return pl.pallas_call(
        attention_kernel,
        grid=(steps,),
        out_shape=(jax.ShapeDtypeStruct((seq_len, HEAD_SIZE), jnp.bfloat16),
                   jax.ShapeDtypeStruct((1, seq_len), jnp.float32),
                   jax.ShapeDtypeStruct((1, seq_len), jnp.float32)),
        in_specs=[rows, whole, whole], out_specs=(rows, line, line),
        scratch_shapes=[pltpu.VMEM((seq_len, BLOCK), jnp.float32), pltpu.VMEM((HEAD_SIZE, BLOCK), jnp.float32)],
        compiler_params=pltpu.CompilerParams(dimension_semantics=("arbitrary",), vmem_limit_bytes=40 << 20),
        cost_estimate=pl.CostEstimate(flops=8 * seq_len * seq_len * HEAD_SIZE, bytes_accessed=8 * seq_len * HEAD_SIZE, transcendentals=0),
    )(q, k, v)


def attention_grad_kernel(q_ref, k_ref, v_ref, do_ref, max_ref, inv_ref, dq_ref, dk_ref, dv_ref, p_scr, dp_scr, dq_scr, dk_scr, dv_scr):
    i = pl.program_id(0)
    q_blk, do_blk = q_ref[...], do_ref[...]
    top, inv = max_ref[...], inv_ref[...]

    @pl.when(i == 0)
    def _():
        dk_scr[...] = jnp.zeros_like(dk_scr)
        dv_scr[...] = jnp.zeros_like(dv_scr)

    def scores(j, mask, delta):
        rows = block_rows(j)
        s = nt(k_ref[rows, :], q_blk) * (ATTN_SCALE * LOG2E)
        if mask is not None:
            s = jnp.where(mask, s, -1e30)
        p = jnp.exp2(s - top) * inv
        dp = nt(v_ref[rows, :], do_blk)
        p_scr[rows, :] = p
        dp_scr[rows, :] = dp
        dv_scr[rows, :] += nn(p.astype(jnp.bfloat16), do_blk)
        return delta + fold_rows(p * dp, jnp.sum)

    delta = scores(i, diagonal_mask(), jnp.zeros((8, BLOCK), jnp.float32))
    delta = lax.fori_loop(0, i, lambda j, d: scores(j, None, d), delta)
    delta = jnp.sum(delta, axis=0, keepdims=True)
    dq_scr[...] = jnp.zeros_like(dq_scr)

    def grads(j, carry):
        rows = block_rows(j)
        ds = (p_scr[rows, :] * (dp_scr[rows, :] - delta) * ATTN_SCALE).astype(jnp.bfloat16)
        dk_scr[rows, :] += nn(ds, q_blk)
        dq_scr[...] += tn(k_ref[rows, :], ds)
        return carry

    lax.fori_loop(0, i + 1, grads, 0)
    dq_ref[...] = dq_scr[...].T

    @pl.when(i == pl.num_programs(0) - 1)
    def _():
        dk_ref[...] = dk_scr[...]
        dv_ref[...] = dv_scr[...].astype(jnp.bfloat16)


def attention_grad(q, k, v, do, top, inv):
    seq_len = q.shape[0]
    steps = seq_len // BLOCK
    rows = pl.BlockSpec((BLOCK, HEAD_SIZE), lambda i: (i, 0))
    whole = pl.BlockSpec((seq_len, HEAD_SIZE), lambda i: (0, 0))
    line = pl.BlockSpec((1, BLOCK), lambda i: (0, i))
    full = (seq_len, HEAD_SIZE)
    return pl.pallas_call(
        attention_grad_kernel,
        grid=(steps,),
        out_shape=(jax.ShapeDtypeStruct(full, jnp.float32), jax.ShapeDtypeStruct(full, jnp.float32), jax.ShapeDtypeStruct(full, jnp.bfloat16)),
        in_specs=[rows, whole, whole, rows, line, line], out_specs=(rows, whole, whole),
        scratch_shapes=[pltpu.VMEM((seq_len, BLOCK), jnp.float32), pltpu.VMEM((seq_len, BLOCK), jnp.float32),
                        pltpu.VMEM((HEAD_SIZE, BLOCK), jnp.float32), pltpu.VMEM(full, jnp.float32), pltpu.VMEM(full, jnp.float32)],
        compiler_params=pltpu.CompilerParams(dimension_semantics=("arbitrary",), vmem_limit_bytes=48 << 20),
        cost_estimate=pl.CostEstimate(flops=20 * seq_len * seq_len * HEAD_SIZE, bytes_accessed=20 * seq_len * HEAD_SIZE, transcendentals=0),
    )(q, k, v, do, top, inv)


COLUMN_GROUPS = [[z * 8 + c * 2 + core for z in range(4) for core in range(2)] for c in range(4)]
PLANE_GROUPS = [[z * 8 + p for p in range(8)] for z in range(4)]


def after_kernel(value_ref, *refs):
    refs[-1][...] = value_ref[...]


def after(value, *others):
    anywhere = pl.BlockSpec(memory_space=pl.ANY)
    return pl.pallas_call(
        after_kernel,
        out_shape=jax.ShapeDtypeStruct(value.shape, value.dtype),
        in_specs=[VMEM] + [anywhere] * len(others), out_specs=VMEM,
        compiler_params=pltpu.CompilerParams(vmem_limit_bytes=8 << 20),
        cost_estimate=pl.CostEstimate(flops=value.size, bytes_accessed=4 * value.size, transcendentals=0),
    )(value, *others)


def lane_rows(values):
    return values.reshape(-1, 128)


def local_block(x_loc, wq_loc, wk_loc, wv_loc, wo_loc, gq_loc, gk_loc, g_attn, dy_loc):
    x_loc, dy_loc = x_loc[0], dy_loc[0]
    rows, model_dim = x_loc.shape
    bf16, f32 = jnp.bfloat16, jnp.float32
    x_full = lax.all_gather(x_loc, 'tp', axis=0, tiled=True)
    seq_len = x_full.shape[0]
    wo_col = lax.all_gather(after(wo_loc, x_full), 'tp', axis=0, tiled=True, axis_index_groups=COLUMN_GROUPS)
    w_rows = jnp.concatenate([wq_loc.T, wk_loc.T, wv_loc.T], axis=0)

    cos_t, sin_t = rope_tables(seq_len)
    q_raw = nn(x_full, wq_loc)
    k_raw = nn(x_full, wk_loc)
    v_head = nn(x_full, wv_loc).astype(bf16)
    stats = jnp.concatenate([lane_rows(jnp.sum(q_raw * q_raw, axis=-1)), lane_rows(jnp.sum(k_raw * k_raw, axis=-1))])
    sq_sums = all_sum(stats, 1).reshape(2, seq_len)
    inv_rms = lax.rsqrt(sq_sums / model_dim + NORM_EPS)[..., None]
    q_unit = q_raw * inv_rms[0]
    k_unit = k_raw * inv_rms[1]
    gq_f, gk_f = gq_loc.astype(f32), gk_loc.astype(f32)
    q_rot = rotate(q_unit * gq_f, cos_t, sin_t).astype(bf16)
    k_rot = rotate(k_unit * gk_f, cos_t, sin_t).astype(bf16)
    o_head, top, inv = attention(q_rot, k_rot, v_head)

    o_col = exchange(
        o_head.reshape(4, 4, 2, rows, HEAD_SIZE), (4, rows, 8 * HEAD_SIZE), column_peer, 8,
        lambda ref, d: ref.at[d // 8, :, lax.rem(d, 2)],
        lambda ref, d: ref.at[:, :, pl.ds(pl.multiple_of(column_of(d)[0] * HEAD_SIZE, HEAD_SIZE), HEAD_SIZE)], 2)
    a_part = nn(o_col.reshape(4 * rows, 8 * HEAD_SIZE), wo_col)
    attn_loc = reduce_scatter(a_part.reshape(4, rows, model_dim), ring_peer, lambda d: lax.rem(d // 2, 4), 3)

    post_rms = lax.rsqrt(jnp.mean(attn_loc * attn_loc, axis=-1, keepdims=True) + NORM_EPS)
    normed = attn_loc * post_rms
    ga_f = g_attn.astype(f32)
    dy_f = dy_loc.astype(f32)
    y_loc = (x_loc.astype(f32) + normed * ga_f).astype(bf16)
    ga_part = jnp.sum(dy_f * normed, axis=0)
    g_normed = dy_f * ga_f
    d_attn = (post_rms * (g_normed - normed * jnp.mean(g_normed * normed, axis=-1, keepdims=True))).astype(bf16)

    d_ring, d_near = spread(d_attn, 4)
    w_plane = lax.all_gather(after(w_rows, d_ring), 'tp', axis=0, tiled=True, axis_index_groups=PLANE_GROUPS)
    d_col = nt(d_ring.reshape(4 * rows, model_dim), wo_col).astype(bf16)
    d_head = exchange(
        d_col.reshape(4, rows, 8 * HEAD_SIZE), (4, 4, 2, rows, HEAD_SIZE), column_peer, 8,
        lambda ref, d: ref.at[:, :, pl.ds(pl.multiple_of(column_of(d)[0] * HEAD_SIZE, HEAD_SIZE), HEAD_SIZE)],
        lambda ref, d: ref.at[d // 8, :, lax.rem(d, 2)], 5).reshape(seq_len, HEAD_SIZE)

    dq_rot, dk_rot, d_value = attention_grad(q_rot, k_rot, v_head, d_head, top, inv)
    dq_hat = rotate_back(dq_rot, cos_t, sin_t)
    dk_hat = rotate_back(dk_rot, cos_t, sin_t)
    grad_gq = jnp.sum(dq_hat * q_unit, axis=0)
    grad_gk = jnp.sum(dk_hat * k_unit, axis=0)
    dq_unit = dq_hat * gq_f
    dk_unit = dk_hat * gk_f
    sums = jnp.concatenate([lane_rows(jnp.sum(dq_unit * q_unit, axis=-1)), lane_rows(jnp.sum(dk_unit * k_unit, axis=-1)), lane_rows(ga_part)])
    sums = all_sum(sums, 6)
    dots_rows = 2 * seq_len // 128
    unit_dots = sums[:dots_rows].reshape(2, seq_len)[..., None] / model_dim
    grad_ga = sums[dots_rows:].reshape(model_dim)
    dq_raw = (inv_rms[0] * (dq_unit - q_unit * unit_dots[0])).astype(bf16)
    dk_raw = (inv_rms[1] * (dk_unit - k_unit * unit_dots[1])).astype(bf16)
    d_qkv = jnp.concatenate([dq_raw, dk_raw, d_value], axis=1)

    width = 3 * HEAD_SIZE
    d_plane, d_far = plane_exchange(d_qkv.reshape(4, 8, rows, width), d_attn, 7)
    dx_part = nn(d_plane.reshape(4 * rows, 8 * width), w_plane)
    dx_loc, grad_w, grad_wo = final(dx_part.reshape(4, rows, model_dim), d_ring, d_near, d_far, d_qkv.T, o_head.T, x_full, 8)
    grad_x = (dx_loc + dy_f).astype(bf16)
    grad_wq, grad_wk, grad_wv = [grad_w[i * HEAD_SIZE:(i + 1) * HEAD_SIZE].T for i in range(3)]
    return (y_loc[None], grad_x[None], grad_wq, grad_wk, grad_wv, grad_wo,
            grad_gq.astype(bf16), grad_gk.astype(bf16), grad_ga.astype(bf16))


def solution(mesh):
    act_spec = P(None, 'tp', None)
    col_spec = P(None, 'tp')
    row_spec = P('tp', None)
    vec_spec = P('tp')
    in_specs = (act_spec, col_spec, col_spec, col_spec, row_spec, vec_spec, vec_spec, P(), act_spec)
    out_specs = (act_spec, act_spec, col_spec, col_spec, col_spec, row_spec, vec_spec, vec_spec, P())
    return jax.shard_map(local_block, mesh=mesh, in_specs=in_specs, out_specs=out_specs, check_vma=False)
```

```python
import functools

import jax
import jax.numpy as jnp
from jax import lax
from jax.experimental import pallas as pl
from jax.experimental.pallas import tpu as pltpu
from jax.sharding import PartitionSpec as P

HEAD_SIZE = 128
ROPE_THETA = 500000.0
NORM_EPS = 1e-6
LOG2E = 1.4426950408889634
ATTN_SCALE = HEAD_SIZE ** -0.5
MESH = pl.DeviceIdType.MESH
VMEM = pl.BlockSpec(memory_space=pltpu.VMEM)
BLOCK = 512


def rope_tables(seq_len):
    half_dim = HEAD_SIZE // 2
    inv_freq = 1.0 / (ROPE_THETA ** (jnp.arange(half_dim, dtype=jnp.float32) / half_dim))
    angles = jnp.arange(seq_len, dtype=jnp.float32)[:, None] * inv_freq[None, :]
    return jnp.cos(angles), jnp.sin(angles)


def rotate(values, cos_t, sin_t):
    lower_half, upper_half = jnp.split(values, 2, axis=-1)
    return jnp.concatenate([lower_half * cos_t - upper_half * sin_t, upper_half * cos_t + lower_half * sin_t], axis=-1)


def rotate_back(values, cos_t, sin_t):
    lower_half, upper_half = jnp.split(values, 2, axis=-1)
    return jnp.concatenate([lower_half * cos_t + upper_half * sin_t, upper_half * cos_t - lower_half * sin_t], axis=-1)


SEMAPHORES = 72
DEPTH = 1024
CHUNKS = 4
TILE = 512
ANY = pl.BlockSpec(memory_space=pl.ANY)


def position(d):
    return d // 8, d // 2 % 4, d % 2


def member_of(d):
    z, _, core = position(d)
    return z * 2 + core


def column_peer(me, k):
    member = (member_of(me) + k) % 8
    return member // 2 * 8 + position(me)[1] * 2 + member % 2


def plane_peer(me, k):
    return me - me % 8 + (me + k) % 8


def ring_peer(me, k):
    z, c, core = position(me)
    return z * 8 + (c + k) % 4 * 2 + core


def line_peer(me, k):
    return (me + k * 8) % 32


def ring_steps(c, core):
    step_x, step_y = 1 - c % 2 * 2, 2 - c // 2 * 4
    step1 = step_x * (1 - core) + step_y * core
    return step1, step_x + step_y - step1


def greet(peers):
    barrier = pltpu.get_barrier_semaphore()
    for peer in peers:
        pl.semaphore_signal(barrier, inc=1, device_id=(peer,), device_id_type=MESH)
    pl.semaphore_wait(barrier, len(peers))


def remote(src, dst, sems, slot, peer):
    return pltpu.make_async_remote_copy(
        src_ref=src, dst_ref=dst, send_sem=sems[0].at[slot], recv_sem=sems[1].at[slot], device_id=(peer,), device_id_type=MESH)


class Copies:
    def __init__(self, sems):
        self.sems, self.used = sems, 0

    def send(self, src, dst, peer):
        copy = remote(src, dst, self.sems, self.used, peer)
        copy.start()
        self.used += 1
        return copy

    def local(self, src, dst):
        copy = pltpu.make_async_copy(src, dst, self.sems[2].at[self.used])
        copy.start()
        self.used += 1
        return copy


def wait_all(copies):
    for copy in copies:
        copy.wait()


def call(kernel, out_shape, operands, in_specs, out_specs, scratch, collective_id, mib):
    return pl.pallas_call(
        kernel, out_shape=out_shape, in_specs=in_specs, out_specs=out_specs,
        scratch_shapes=list(scratch) + [pltpu.SemaphoreType.DMA((SEMAPHORES,))] * 3,
        compiler_params=pltpu.CompilerParams(collective_id=collective_id, has_side_effects=True, vmem_limit_bytes=mib << 20),
    )(*operands)


def shape(dims, dtype):
    return jax.ShapeDtypeStruct(tuple(dims), dtype)


def part(index, size):
    return pl.ds(pl.multiple_of(index * size, size), size)


def add_rows(ref, other, start, count):
    def add(i, carry):
        rows = part(start // 8 + i, 8)
        ref[rows, :] = ref[rows, :] + other[rows, :]
        return carry

    lax.fori_loop(0, count // 8, add, 0)


def exchange_kernel(peer_of, count, source, target, x_ref, out_ref, *sems):
    me, copies = lax.axis_index('tp'), Copies(sems)
    peers = [peer_of(me, k) for k in range(1, count)]
    greet(peers)
    started = [copies.send(source(x_ref, peer), target(out_ref, me), peer) for peer in peers]
    target(out_ref, me)[...] = source(x_ref, me)[...]
    wait_all(started)


def exchange(x, out_shape, peer_of, count, source, target, collective_id):
    kernel = functools.partial(exchange_kernel, peer_of, count, source, target)
    return call(kernel, shape(out_shape, x.dtype), (x,), [VMEM], VMEM, [], collective_id, 24)


def all_sum_kernel(x_ref, out_ref, plane, middle, line, *sems):
    me, copies = lax.axis_index('tp'), Copies(sems)
    z, mine = me // 8, me % 8
    plane_peers = [plane_peer(me, k) for k in range(1, 8)]
    line_peers = [line_peer(me, k) for k in range(1, 4)]
    greet(plane_peers + line_peers)
    started = [copies.send(x_ref, plane.at[mine], peer) for peer in plane_peers]
    plane[mine] = x_ref[...]
    wait_all(started)
    total = plane[0]
    for k in range(1, 8):
        total = total + plane[k]
    middle[...] = total
    line[z] = total
    wait_all([copies.send(middle, line.at[z], peer) for peer in line_peers])
    out_ref[...] = (line[0] + line[1]) + (line[2] + line[3])


def all_sum(x, collective_id):
    scratch = [pltpu.VMEM((8,) + x.shape, x.dtype), pltpu.VMEM(x.shape, x.dtype), pltpu.VMEM((4,) + x.shape, x.dtype)]
    return call(all_sum_kernel, shape(x.shape, x.dtype), (x,), [VMEM], VMEM, scratch, collective_id, 8)


def ring_sum_kernel(x_ref, out_ref, passing, direct, last, *sems):
    me, copies = lax.axis_index('tp'), Copies(sems)
    _, c, core = position(me)
    step1, step2 = ring_steps(c, core)
    first, second = me + step1 * 2, me + step2 * 2
    greet([first, second])
    chunk = out_ref.shape[0] // CHUNKS
    pieces = [pl.ds(i * chunk, chunk) for i in range(CHUNKS)]
    hops = [copies.send(x_ref.at[c + step1 + step2, p, :], passing.at[p, :], first) for p in pieces]
    sums = [copies.send(x_ref.at[c + step1], direct, first)]
    for i, p in enumerate(pieces):
        hops[i].wait()
        add_rows(passing, x_ref.at[c + step2], i * chunk, chunk)
        sums.append(copies.send(passing.at[p, :], last.at[p, :], second))
    wait_all(sums)

    def add(i, carry):
        rows = part(i, 8)
        out_ref[rows, :] = (x_ref[c, rows, :] + direct[rows, :]) + last[rows, :]
        return carry

    lax.fori_loop(0, out_ref.shape[0] // 8, add, 0)


def ring_sum(x, collective_id):
    dims = x.shape[1:]
    return call(ring_sum_kernel, shape(dims, x.dtype), (x,), [VMEM], VMEM, [pltpu.VMEM(dims, x.dtype)] * 3, collective_id, 32)


def spread_kernel(x_ref, ring_ref, near_ref, *sems):
    me, copies = lax.axis_index('tp'), Copies(sems)
    ring = [ring_peer(me, k) for k in range(1, 4)]
    line = [line_peer(me, k) for k in (1, 3)]
    greet(ring + line)
    mine = position(me)[1]
    started = [copies.send(x_ref, ring_ref.at[mine], peer) for peer in ring]
    started += [copies.send(x_ref, near_ref.at[i], peer) for i, peer in enumerate(line)]
    ring_ref[mine] = x_ref[...]
    wait_all(started)


def spread(x, collective_id):
    out = (shape((4,) + x.shape, x.dtype), shape((2,) + x.shape, x.dtype))
    return call(spread_kernel, out, (x,), [VMEM], (VMEM, VMEM), [], collective_id, 24)


def plane_kernel(qk_ref, v_ref, near_ref, out_qk, out_v, far_ref, *sems):
    me, copies = lax.axis_index('tp'), Copies(sems)
    peers = [plane_peer(me, k) for k in range(1, 8)]
    up, down = line_peer(me, 1), line_peer(me, 3)
    greet(peers + [up, down])
    mine = me % 8
    started = [copies.send(near_ref.at[0], far_ref, up)]
    for src, dst in ((qk_ref, out_qk), (v_ref, out_v)):
        columns = part(mine, src.shape[-1])
        started += [copies.send(src.at[:, peer % 8], dst.at[:, :, columns], peer) for peer in peers]
        dst[:, :, columns] = src[:, mine]
    wait_all(started)


def plane_exchange(qk, v, near, collective_id):
    outs = tuple(shape((4, a.shape[2], 8 * a.shape[3]), a.dtype) for a in (qk, v)) + (shape(near.shape[1:], near.dtype),)
    return call(plane_kernel, outs, (qk, v, near), [VMEM, VMEM, ANY], (VMEM, VMEM, VMEM), [], collective_id, 24)


def final_kernel(dqk_ref, dv_ref, wqk_ref, wv_ref, ring_ref, near_ref, far_ref, dw_ref, o_ref, x_ref, sum_ref, gw_ref, gwo_ref,
                 dx, above, below, passing, full, buf, tile_sem, line_send, line_recv, *sems):
    me, copies = lax.axis_index('tp'), Copies(sems)
    z, c, core = position(me)
    partner = me + 1 - core * 2
    up, down = line_peer(me, 1), line_peer(me, 3)
    z_up, z_far, z_down = up // 8, line_peer(me, 2) // 8, down // 8
    ring = [ring_peer(me, k) for k in range(1, 4)]
    greet([up, down, partner] + ring)
    tiles = x_ref.shape[1] // TILE
    depth = dqk_ref.shape[1]
    line_sems = (line_send, line_recv)

    def fetch_w(j, b):
        return [pltpu.make_async_copy(wqk_ref.at[:, part(j, TILE)], buf.at[b, pl.ds(0, depth), :], tile_sem.at[0, b]),
                pltpu.make_async_copy(wv_ref.at[:, part(j, TILE)], buf.at[b, pl.ds(depth, dv_ref.shape[1]), :], tile_sem.at[1, b])]

    def fetch_x(j, b):
        return [pltpu.make_async_copy(x_ref.at[:, part(j, TILE)], buf.at[b], tile_sem.at[0, b])]

    for copy in fetch_w(0, 0):
        copy.start()
    planes, lines = [z_down, z_up, z_far], [near_ref.at[0], near_ref.at[1], far_ref]

    def slot(plane, column):
        return full.at[plane * 8 + column * 2 + core]

    rounds, shared, local = [], [], []
    for plane, block in zip(planes, lines):
        rounds += [copies.send(block, slot(plane, c), peer) for peer in ring]
    held = [(block, slot(plane, c)) for plane, block in zip(planes, lines)]
    held += [(ring_ref.at[column], slot(z, column)) for column in range(4)]
    for block, place in held:
        shared.append(copies.send(block, place, partner))
        local.append(copies.local(block, place))

    def hop(j):
        return remote(dx.at[z_far, :, part(j, TILE)], passing.at[:, part(j, TILE)], line_sems, j, up)

    def direct(j):
        return remote(dx.at[z_down, :, part(j, TILE)], above.at[:, part(j, TILE)], line_sems, tiles + j, down)

    def onward(j):
        return remote(passing.at[:, part(j, TILE)], below.at[:, part(j, TILE)], line_sems, tiles * 2 + j, up)

    def input_grad(j, carry):
        b = j % 2

        @pl.when(j + 1 < tiles)
        def _():
            for copy in fetch_w(j + 1, 1 - b):
                copy.start()

        wait_all(fetch_w(j, b))
        values = nn(dqk_ref[...], buf[b, :depth, :]) + nn(dv_ref[...], buf[b, depth:, :])
        dx[:, :, part(j, TILE)] = values.reshape(dx.shape[0], dx.shape[1], TILE)

        @pl.when(j > 0)
        def _():
            hop(j - 1).start()
            direct(j - 1).start()

        return carry

    lax.fori_loop(0, tiles, input_grad, 0)
    for copy in fetch_x(0, 0):
        copy.start()

    def weight_grad(j, carry):
        b = j % 2

        @pl.when(j + 1 < tiles)
        def _():
            for copy in fetch_x(j + 1, 1 - b):
                copy.start()

        wait_all(fetch_x(j, b))

        @pl.when(j == 0)
        def _():
            hop(tiles - 1).start()
            direct(tiles - 1).start()

        hop(j).wait()
        passing[:, part(j, TILE)] = passing[:, part(j, TILE)] + dx[z_up, :, part(j, TILE)]
        gw_ref[:, part(j, TILE)] = nn(dw_ref[...], buf[b]).astype(gw_ref.dtype)
        onward(j).start()
        return carry

    lax.fori_loop(0, tiles, weight_grad, 0)
    for i, copy in enumerate(rounds):
        copy.wait()
        block = slot(planes[i // 3], (c + 3 - i % 3) % 4)
        shared.append(copies.send(block, block, partner))

    def finish(j, carry):
        direct(j).wait()
        onward(j).wait()
        tile = part(j, TILE)
        sum_ref[:, tile] = (dx[z, :, tile] + above[:, tile]) + below[:, tile]
        return carry

    lax.fori_loop(0, tiles, finish, 0)
    wait_all(local + shared)

    def out_grad(j, carry):
        d = full[:, :, part(j, TILE)]
        gwo_ref[:, part(j, TILE)] = nn(o_ref[...], d.reshape(o_ref.shape[1], TILE)).astype(gwo_ref.dtype)
        return carry

    lax.fori_loop(0, tiles, out_grad, 0)


def final(dqk, dv, wqk, wv, d_ring, d_near, d_far, dw_rows, o_rows, x_full, collective_id):
    rows, model_dim = d_far.shape
    seq_len = x_full.shape[0]
    bf16, f32 = d_far.dtype, jnp.float32
    block = pltpu.VMEM((rows, model_dim), f32)
    scratch = [pltpu.VMEM((dqk.shape[0] // rows, rows, model_dim), f32), block, block, block,
               pltpu.VMEM((seq_len // rows, rows, model_dim), bf16), pltpu.VMEM((2, seq_len, TILE), bf16), pltpu.SemaphoreType.DMA((2, 2)),
               pltpu.SemaphoreType.DMA((SEMAPHORES,)), pltpu.SemaphoreType.DMA((SEMAPHORES,))]
    outs = (shape(d_far.shape, f32), shape((dw_rows.shape[0], model_dim), bf16), shape((o_rows.shape[0], model_dim), bf16))
    return call(final_kernel, outs, (dqk, dv, wqk, wv, d_ring, d_near, d_far, dw_rows, o_rows, x_full),
                [VMEM, VMEM, ANY, ANY, ANY, ANY, ANY, VMEM, VMEM, ANY], (VMEM, VMEM, VMEM),
                scratch, collective_id, 60)


def gather_kernel(x_ref, wq_ref, wk_ref, wv_ref, wo_ref, out_ref, q_ref, k_ref, v_ref, col_ref,
                  full, weights, total, *sems):
    me, copies = lax.axis_index('tp'), Copies(sems)
    z, c, core = position(me)
    partner = me + 1 - core * 2
    step1, step2 = ring_steps(c, core)
    first, second = me + step1 * 2, me + step2 * 2
    up, far, down = [line_peer(me, k) for k in range(1, 4)]
    planes = [z, down // 8, up // 8, far // 8]
    direct, corner = (0, 1, 3, 5), (2, 4, 6, 7)

    def slot(plane, column):
        return full.at[plane * 8 + column * 2 + core]

    own = copies.local(x_ref, slot(z, c))
    loads = [copies.local(ref, weights.at[:, pl.ds(i * HEAD_SIZE, HEAD_SIZE)]) for i, ref in enumerate((wq_ref, wk_ref, wv_ref))]
    greet([up, down, first, second, partner])
    own.wait()
    line = {i: copies.send(slot(z, c), slot(z, c), peer) for i, peer in ((1, up), (2, down))}
    to_first, to_second, to_partner, stores = {}, {}, {}, []

    def forward(s, column, index, slot_of):
        block = slot(planes[s], column)
        if index is not None:
            to_second[index] = copies.send(block, block, second)
        to_partner[slot_of] = copies.send(block, block, partner)

    def pass_on(s):
        block = slot(planes[s], c)
        to_first[s] = copies.send(block, block, first)
        forward(s, c, direct[s], s)

    def from_line(s):
        line[s].wait()
        pass_on(s)

    head, head_line, head_partner = (lambda plane: col_ref.at[plane * 2 + core]), {}, []

    def head_from_line(s):
        head_line[s].wait()
        block = head(planes[s])
        if s == 1:
            head_line[3] = copies.send(block, block, up)
        head_partner.append(copies.send(block, block, partner))

    def from_first(s):
        to_first[s].wait()
        forward(s, c + step1, corner[s], 4 + s)

    def from_second(i):
        to_second[i].wait()
        if i in direct:
            forward(direct.index(i), c + step2, None, 8 + i)
        else:
            forward(corner.index(i), c + step2 + step1, None, 8 + i)

    def multiply(s, column, slot_of):
        to_partner[slot_of].wait()
        pair = planes[s] * 4 + column
        blocks = pl.ds(pair * 2, 2)
        stores.append(copies.local(full.at[blocks], out_ref.at[blocks]))
        rows = part(pair, total.shape[0])
        total[...] = jnp.zeros_like(total)

        def chunk(i, carry):
            depth = part(i, DEPTH)
            a = full[blocks, :, depth].reshape(rows.size, DEPTH)
            total[...] += nn(a, weights[depth, :])
            return carry

        lax.fori_loop(0, weights.shape[0] // DEPTH, chunk, 0)
        q_ref[rows, :] = total[:, :HEAD_SIZE]
        k_ref[rows, :] = total[:, HEAD_SIZE:2 * HEAD_SIZE]
        v_ref[rows, :] = total[:, 2 * HEAD_SIZE:].astype(v_ref.dtype)

    def multiply_own(s):
        multiply(s, c, s)

    def multiply_sides(s):
        multiply(s, c + step1, 8 + direct[s])
        multiply(s, c + step2, 4 + s)

    def multiply_corner(s):
        multiply(s, c + step1 + step2, 8 + corner[s])

    pass_on(0)
    from_line(1)
    line[3] = copies.send(slot(planes[1], c), slot(planes[1], c), up)
    own_head = copies.local(wo_ref, head(z))
    head_line[1] = copies.send(wo_ref, head(z), up)
    head_line[2] = copies.send(wo_ref, head(z), down)
    head_partner.append(copies.send(wo_ref, head(z), partner))
    from_first(0)
    wait_all(loads)
    multiply_own(0)
    from_second(0)
    from_line(2)
    from_first(1)
    multiply_own(1)
    from_second(1)
    from_first(2)
    from_line(3)
    multiply_own(2)
    from_second(2)
    head_from_line(1)
    multiply_sides(0)
    from_first(3)
    multiply_own(3)
    from_second(3)
    multiply_sides(1)
    from_second(4)
    multiply_corner(0)
    from_second(5)
    multiply_sides(2)
    head_from_line(2)
    from_second(6)
    multiply_sides(3)
    multiply_corner(1)
    from_second(7)
    multiply_corner(2)
    multiply_corner(3)
    head_from_line(3)
    wait_all(stores + [own_head] + head_partner)


def gather(x, wq, wk, wv, wo, devices, collective_id):
    rows, model_dim = x.shape
    f32 = jnp.float32
    head = (devices * rows, HEAD_SIZE)
    outs = (shape((devices, rows, model_dim), x.dtype), shape(head, f32), shape(head, f32), shape(head, x.dtype),
            shape((8,) + wo.shape, wo.dtype))
    width = 3 * HEAD_SIZE
    scratch = [pltpu.VMEM((devices, rows, model_dim), x.dtype), pltpu.VMEM((model_dim, width), x.dtype), pltpu.VMEM((2 * rows, width), f32)]
    return call(gather_kernel, outs, (x, wq, wk, wv, wo), [ANY] * 5, (ANY, VMEM, VMEM, VMEM, ANY), scratch, collective_id, 44)


def nt(a, b):
    return lax.dot_general(a, b, (((1,), (1,)), ((), ())), preferred_element_type=jnp.float32)


def tn(a, b):
    return lax.dot_general(a, b, (((0,), (0,)), ((), ())), preferred_element_type=jnp.float32)


def nn(a, b):
    return lax.dot_general(a, b, (((1,), (0,)), ((), ())), preferred_element_type=jnp.float32)


def fold_rows(values, op):
    return op(values.reshape(values.shape[0] // 8, 8, values.shape[1]), axis=0)


def block_rows(j):
    return pl.ds(pl.multiple_of(j * BLOCK, BLOCK), BLOCK)


def diagonal_mask():
    keys = lax.broadcasted_iota(jnp.int32, (BLOCK, BLOCK), 0)
    queries = lax.broadcasted_iota(jnp.int32, (BLOCK, BLOCK), 1)
    return keys <= queries


def attention_kernel(q_ref, k_ref, v_ref, o_ref, max_ref, inv_ref, s_scr, acc_scr):
    i = pl.program_id(0)
    q_blk = q_ref[...]

    def score(j, top):
        s = nt(k_ref[block_rows(j), :], q_blk) * (ATTN_SCALE * LOG2E)
        s_scr[block_rows(j), :] = s
        return jnp.maximum(top, fold_rows(s, jnp.max))

    s = jnp.where(diagonal_mask(), nt(k_ref[block_rows(i), :], q_blk) * (ATTN_SCALE * LOG2E), -1e30)
    s_scr[block_rows(i), :] = s
    top = lax.fori_loop(0, i, score, fold_rows(s, jnp.max))
    top = jnp.max(top, axis=0, keepdims=True)

    def weigh(j, total):
        p = jnp.exp2(s_scr[block_rows(j), :] - top)
        s_scr[block_rows(j), :] = p
        return total + fold_rows(p, jnp.sum)

    total = lax.fori_loop(0, i + 1, weigh, jnp.zeros((8, BLOCK), jnp.float32))
    inv = 1.0 / jnp.sum(total, axis=0, keepdims=True)
    max_ref[...] = top
    inv_ref[...] = inv
    acc_scr[...] = jnp.zeros_like(acc_scr)

    def gather(j, carry):
        p = (s_scr[block_rows(j), :] * inv).astype(jnp.bfloat16)
        acc_scr[...] += tn(v_ref[block_rows(j), :], p)
        return carry

    lax.fori_loop(0, i + 1, gather, 0)
    o_ref[...] = acc_scr[...].T.astype(jnp.bfloat16)


def attention(q, k, v):
    seq_len = q.shape[0]
    steps = seq_len // BLOCK
    rows = pl.BlockSpec((BLOCK, HEAD_SIZE), lambda i: (i, 0))
    whole = pl.BlockSpec((seq_len, HEAD_SIZE), lambda i: (0, 0))
    line = pl.BlockSpec((1, BLOCK), lambda i: (0, i))
    return pl.pallas_call(
        attention_kernel,
        grid=(steps,),
        out_shape=(jax.ShapeDtypeStruct((seq_len, HEAD_SIZE), jnp.bfloat16),
                   jax.ShapeDtypeStruct((1, seq_len), jnp.float32),
                   jax.ShapeDtypeStruct((1, seq_len), jnp.float32)),
        in_specs=[rows, whole, whole], out_specs=(rows, line, line),
        scratch_shapes=[pltpu.VMEM((seq_len, BLOCK), jnp.float32), pltpu.VMEM((HEAD_SIZE, BLOCK), jnp.float32)],
        compiler_params=pltpu.CompilerParams(dimension_semantics=("arbitrary",), vmem_limit_bytes=40 << 20),
        cost_estimate=pl.CostEstimate(flops=8 * seq_len * seq_len * HEAD_SIZE, bytes_accessed=8 * seq_len * HEAD_SIZE, transcendentals=0),
    )(q, k, v)


def attention_grad_kernel(q_ref, k_ref, v_ref, do_ref, max_ref, inv_ref, dq_ref, dk_ref, dv_ref, p_scr, dp_scr, dq_scr, dk_scr, dv_scr):
    i = pl.program_id(0)
    q_blk, do_blk = q_ref[...], do_ref[...]
    top, inv = max_ref[...], inv_ref[...]

    @pl.when(i == 0)
    def _():
        dk_scr[...] = jnp.zeros_like(dk_scr)
        dv_scr[...] = jnp.zeros_like(dv_scr)

    def scores(j, mask, delta):
        rows = block_rows(j)
        s = nt(k_ref[rows, :], q_blk) * (ATTN_SCALE * LOG2E)
        if mask is not None:
            s = jnp.where(mask, s, -1e30)
        p = jnp.exp2(s - top) * inv
        dp = nt(v_ref[rows, :], do_blk)
        p_scr[rows, :] = p
        dp_scr[rows, :] = dp
        dv_scr[rows, :] += nn(p.astype(jnp.bfloat16), do_blk)
        return delta + fold_rows(p * dp, jnp.sum)

    delta = scores(i, diagonal_mask(), jnp.zeros((8, BLOCK), jnp.float32))
    delta = lax.fori_loop(0, i, lambda j, d: scores(j, None, d), delta)
    delta = jnp.sum(delta, axis=0, keepdims=True)
    dq_scr[...] = jnp.zeros_like(dq_scr)

    def grads(j, carry):
        rows = block_rows(j)
        ds = (p_scr[rows, :] * (dp_scr[rows, :] - delta) * ATTN_SCALE).astype(jnp.bfloat16)
        dk_scr[rows, :] += nn(ds, q_blk)
        dq_scr[...] += tn(k_ref[rows, :], ds)
        return carry

    lax.fori_loop(0, i + 1, grads, 0)
    dq_ref[...] = dq_scr[...].T

    @pl.when(i == pl.num_programs(0) - 1)
    def _():
        dk_ref[...] = dk_scr[...]
        dv_ref[...] = dv_scr[...].astype(jnp.bfloat16)


def attention_grad(q, k, v, do, top, inv):
    seq_len = q.shape[0]
    steps = seq_len // BLOCK
    rows = pl.BlockSpec((BLOCK, HEAD_SIZE), lambda i: (i, 0))
    whole = pl.BlockSpec((seq_len, HEAD_SIZE), lambda i: (0, 0))
    line = pl.BlockSpec((1, BLOCK), lambda i: (0, i))
    full = (seq_len, HEAD_SIZE)
    return pl.pallas_call(
        attention_grad_kernel,
        grid=(steps,),
        out_shape=(jax.ShapeDtypeStruct(full, jnp.float32), jax.ShapeDtypeStruct(full, jnp.float32), jax.ShapeDtypeStruct(full, jnp.bfloat16)),
        in_specs=[rows, whole, whole, rows, line, line], out_specs=(rows, whole, whole),
        scratch_shapes=[pltpu.VMEM((seq_len, BLOCK), jnp.float32), pltpu.VMEM((seq_len, BLOCK), jnp.float32),
                        pltpu.VMEM((HEAD_SIZE, BLOCK), jnp.float32), pltpu.VMEM(full, jnp.float32), pltpu.VMEM(full, jnp.float32)],
        compiler_params=pltpu.CompilerParams(dimension_semantics=("arbitrary",), vmem_limit_bytes=48 << 20),
        cost_estimate=pl.CostEstimate(flops=20 * seq_len * seq_len * HEAD_SIZE, bytes_accessed=20 * seq_len * HEAD_SIZE, transcendentals=0),
    )(q, k, v, do, top, inv)


COLUMN_GROUPS = [[z * 8 + c * 2 + core for z in range(4) for core in range(2)] for c in range(4)]
PLANE_GROUPS = [[z * 8 + p for p in range(8)] for z in range(4)]


def after_kernel(value_ref, *refs):
    refs[-1][...] = value_ref[...]


def after(value, *others):
    anywhere = pl.BlockSpec(memory_space=pl.ANY)
    return pl.pallas_call(
        after_kernel,
        out_shape=jax.ShapeDtypeStruct(value.shape, value.dtype),
        in_specs=[VMEM] + [anywhere] * len(others), out_specs=VMEM,
        compiler_params=pltpu.CompilerParams(vmem_limit_bytes=8 << 20),
        cost_estimate=pl.CostEstimate(flops=value.size, bytes_accessed=4 * value.size, transcendentals=0),
    )(value, *others)


def lane_rows(values):
    return values.reshape(-1, 128)


def local_block(x_loc, wq_loc, wk_loc, wv_loc, wo_loc, gq_loc, gk_loc, g_attn, dy_loc):
    x_loc, dy_loc = x_loc[0], dy_loc[0]
    rows, model_dim = x_loc.shape
    bf16, f32 = jnp.bfloat16, jnp.float32
    x_blocks, q_raw, k_raw, v_head, wo_blocks = gather(x_loc, wq_loc, wk_loc, wv_loc, wo_loc, 32, 9)
    wo_col = wo_blocks.reshape(8 * HEAD_SIZE, model_dim)
    x_full = x_blocks.reshape(32 * rows, model_dim)
    seq_len = x_full.shape[0]
    wv_plane = lax.all_gather(after(wv_loc.T, q_raw[:8]), 'tp', axis=0, tiled=True, axis_index_groups=PLANE_GROUPS)
    cos_t, sin_t = rope_tables(seq_len)
    stats = jnp.concatenate([lane_rows(jnp.sum(q_raw * q_raw, axis=-1)), lane_rows(jnp.sum(k_raw * k_raw, axis=-1))])
    sq_sums = all_sum(stats, 1).reshape(2, seq_len)
    inv_rms = lax.rsqrt(sq_sums / model_dim + NORM_EPS)[..., None]
    q_unit = q_raw * inv_rms[0]
    k_unit = k_raw * inv_rms[1]
    gq_f, gk_f = gq_loc.astype(f32), gk_loc.astype(f32)
    q_rot = rotate(q_unit * gq_f, cos_t, sin_t).astype(bf16)
    k_rot = rotate(k_unit * gk_f, cos_t, sin_t).astype(bf16)
    o_head, top, inv = attention(q_rot, k_rot, v_head)

    o_col = exchange(
        o_head.reshape(4, 4, 2, rows, HEAD_SIZE), (4, rows, 8 * HEAD_SIZE), column_peer, 8,
        lambda ref, d: ref.at[d // 8, :, d % 2],
        lambda ref, d: ref.at[:, :, part(member_of(d), HEAD_SIZE)], 2)
    a_part = nn(o_col.reshape(4 * rows, 8 * HEAD_SIZE), wo_col)
    attn_loc = ring_sum(a_part.reshape(4, rows, model_dim), 3)

    post_rms = lax.rsqrt(jnp.mean(attn_loc * attn_loc, axis=-1, keepdims=True) + NORM_EPS)
    normed = attn_loc * post_rms
    ga_f = g_attn.astype(f32)
    dy_f = dy_loc.astype(f32)
    y_loc = (x_loc.astype(f32) + normed * ga_f).astype(bf16)
    ga_part = jnp.sum(dy_f * normed, axis=0)
    g_normed = dy_f * ga_f
    d_attn = (post_rms * (g_normed - normed * jnp.mean(g_normed * normed, axis=-1, keepdims=True))).astype(bf16)

    d_ring, d_near = spread(d_attn, 4)
    wqk_plane = lax.all_gather(after(jnp.concatenate([wq_loc.T, wk_loc.T], axis=0), d_ring), 'tp', axis=0, tiled=True, axis_index_groups=PLANE_GROUPS)
    d_col = nt(d_ring.reshape(4 * rows, model_dim), wo_col).astype(bf16)
    d_head = exchange(
        d_col.reshape(4, rows, 8 * HEAD_SIZE), (4, 4, 2, rows, HEAD_SIZE), column_peer, 8,
        lambda ref, d: ref.at[:, :, part(member_of(d), HEAD_SIZE)],
        lambda ref, d: ref.at[d // 8, :, d % 2], 5).reshape(seq_len, HEAD_SIZE)

    dq_rot, dk_rot, d_value = attention_grad(q_rot, k_rot, v_head, d_head, top, inv)
    dq_hat = rotate_back(dq_rot, cos_t, sin_t)
    dk_hat = rotate_back(dk_rot, cos_t, sin_t)
    grad_gq = jnp.sum(dq_hat * q_unit, axis=0)
    grad_gk = jnp.sum(dk_hat * k_unit, axis=0)
    dq_unit = dq_hat * gq_f
    dk_unit = dk_hat * gk_f
    sums = jnp.concatenate([lane_rows(jnp.sum(dq_unit * q_unit, axis=-1)), lane_rows(jnp.sum(dk_unit * k_unit, axis=-1)), lane_rows(ga_part)])
    sums = all_sum(sums, 6)
    dots_rows = 2 * seq_len // 128
    unit_dots = sums[:dots_rows].reshape(2, seq_len)[..., None] / model_dim
    grad_ga = sums[dots_rows:].reshape(model_dim)
    dq_raw = (inv_rms[0] * (dq_unit - q_unit * unit_dots[0])).astype(bf16)
    dk_raw = (inv_rms[1] * (dk_unit - k_unit * unit_dots[1])).astype(bf16)
    d_qk = jnp.concatenate([dq_raw, dk_raw], axis=1)
    dw_rows = jnp.concatenate([dq_raw.T, dk_raw.T, d_value.T], axis=0)

    dqk_plane, dv_plane, d_far = plane_exchange(
        d_qk.reshape(4, 8, rows, 2 * HEAD_SIZE), d_value.reshape(4, 8, rows, HEAD_SIZE), d_near, 7)
    dx_loc, grad_w, grad_wo = final(
        dqk_plane.reshape(4 * rows, 16 * HEAD_SIZE), dv_plane.reshape(4 * rows, 8 * HEAD_SIZE), wqk_plane, wv_plane,
        d_ring, d_near, d_far, dw_rows, o_head.T, x_full, 8)
    grad_x = (dx_loc + dy_f).astype(bf16)
    grad_wq, grad_wk, grad_wv = [grad_w[i * HEAD_SIZE:(i + 1) * HEAD_SIZE].T for i in range(3)]
    return (y_loc[None], grad_x[None], grad_wq, grad_wk, grad_wv, grad_wo,
            grad_gq.astype(bf16), grad_gk.astype(bf16), grad_ga.astype(bf16))


def solution(mesh):
    act_spec = P(None, 'tp', None)
    col_spec = P(None, 'tp')
    row_spec = P('tp', None)
    vec_spec = P('tp')
    in_specs = (act_spec, col_spec, col_spec, col_spec, row_spec, vec_spec, vec_spec, P(), act_spec)
    out_specs = (act_spec, act_spec, col_spec, col_spec, col_spec, row_spec, vec_spec, vec_spec, P())
    return jax.shard_map(local_block, mesh=mesh, in_specs=in_specs, out_specs=out_specs, check_vma=False)
```

```python
import functools

import jax
import jax.numpy as jnp
from jax import lax
from jax.experimental import pallas as pl
from jax.experimental.pallas import tpu as pltpu
from jax.sharding import PartitionSpec as P

HEAD_SIZE = 128
ROPE_THETA = 500000.0
NORM_EPS = 1e-6
LOG2E = 1.4426950408889634
ATTN_SCALE = HEAD_SIZE ** -0.5
MESH = pl.DeviceIdType.MESH
VMEM = pl.BlockSpec(memory_space=pltpu.VMEM)
BLOCK = 512


def rope_tables(seq_len):
    half_dim = HEAD_SIZE // 2
    inv_freq = 1.0 / (ROPE_THETA ** (jnp.arange(half_dim, dtype=jnp.float32) / half_dim))
    angles = inv_freq[:, None] * jnp.arange(seq_len, dtype=jnp.float32)[None, :]
    return jnp.cos(angles), jnp.sin(angles)


def rotate(values, cos_t, sin_t):
    lower_half, upper_half = jnp.split(values, 2, axis=0)
    return jnp.concatenate([lower_half * cos_t - upper_half * sin_t, upper_half * cos_t + lower_half * sin_t], axis=0)


def rotate_back(values, cos_t, sin_t):
    return rotate(values, cos_t, -sin_t)


SEMAPHORES = 72
DEPTH = 1024
CHUNKS = 4
TILE = 512
ANY = pl.BlockSpec(memory_space=pl.ANY)


def position(d):
    return d // 8, d // 2 % 4, d % 2


def member_of(d):
    z, _, core = position(d)
    return z * 2 + core


def column_peer(me, k):
    member = (member_of(me) + k) % 8
    return member // 2 * 8 + position(me)[1] * 2 + member % 2


def plane_peer(me, k):
    return me - me % 8 + (me + k) % 8


def ring_peer(me, k):
    z, c, core = position(me)
    return z * 8 + (c + k) % 4 * 2 + core


def line_peer(me, k):
    return (me + k * 8) % 32


def ring_steps(c, core):
    step_x, step_y = 1 - c % 2 * 2, 2 - c // 2 * 4
    step1 = step_x * (1 - core) + step_y * core
    return step1, step_x + step_y - step1


def greet(peers):
    barrier = pltpu.get_barrier_semaphore()
    for peer in peers:
        pl.semaphore_signal(barrier, inc=1, device_id=(peer,), device_id_type=MESH)
    pl.semaphore_wait(barrier, len(peers))


def remote(src, dst, sems, slot, peer):
    return pltpu.make_async_remote_copy(
        src_ref=src, dst_ref=dst, send_sem=sems[0].at[slot], recv_sem=sems[1].at[slot], device_id=(peer,), device_id_type=MESH)


class Copies:
    def __init__(self, sems):
        self.sems, self.used = sems, 0

    def send(self, src, dst, peer):
        copy = remote(src, dst, self.sems, self.used, peer)
        copy.start()
        self.used += 1
        return copy

    def local(self, src, dst):
        copy = pltpu.make_async_copy(src, dst, self.sems[2].at[self.used])
        copy.start()
        self.used += 1
        return copy


def wait_all(copies):
    for copy in copies:
        copy.wait()


def call(kernel, out_shape, operands, in_specs, out_specs, scratch, collective_id, mib):
    return pl.pallas_call(
        kernel, out_shape=out_shape, in_specs=in_specs, out_specs=out_specs,
        scratch_shapes=list(scratch) + [pltpu.SemaphoreType.DMA((SEMAPHORES,))] * 3,
        compiler_params=pltpu.CompilerParams(collective_id=collective_id, has_side_effects=True, vmem_limit_bytes=mib << 20),
    )(*operands)


def shape(dims, dtype):
    return jax.ShapeDtypeStruct(tuple(dims), dtype)


def part(index, size):
    return pl.ds(pl.multiple_of(index * size, size), size)


def add_rows(ref, other, start, count):
    def add(i, carry):
        rows = part(start // 8 + i, 8)
        ref[rows, :] = ref[rows, :] + other[rows, :]
        return carry

    lax.fori_loop(0, count // 8, add, 0)


def exchange_kernel(peer_of, count, source, target, x_ref, out_ref, *sems):
    me, copies = lax.axis_index('tp'), Copies(sems)
    peers = [peer_of(me, k) for k in range(1, count)]
    greet(peers)
    started = [copies.send(source(x_ref, peer), target(out_ref, me), peer) for peer in peers]
    target(out_ref, me)[...] = source(x_ref, me)[...]
    wait_all(started)


def exchange(x, out_shape, peer_of, count, source, target, collective_id):
    kernel = functools.partial(exchange_kernel, peer_of, count, source, target)
    return call(kernel, shape(out_shape, x.dtype), (x,), [VMEM], VMEM, [], collective_id, 24)


def all_sum_kernel(x_ref, out_ref, plane, middle, line, *sems):
    me, copies = lax.axis_index('tp'), Copies(sems)
    z, mine = me // 8, me % 8
    plane_peers = [plane_peer(me, k) for k in range(1, 8)]
    line_peers = [line_peer(me, k) for k in range(1, 4)]
    greet(plane_peers + line_peers)
    started = [copies.send(x_ref, plane.at[mine], peer) for peer in plane_peers]
    plane[mine] = x_ref[...]
    wait_all(started)
    total = plane[0]
    for k in range(1, 8):
        total = total + plane[k]
    middle[...] = total
    line[z] = total
    wait_all([copies.send(middle, line.at[z], peer) for peer in line_peers])
    out_ref[...] = (line[0] + line[1]) + (line[2] + line[3])


def all_sum(x, collective_id):
    scratch = [pltpu.VMEM((8,) + x.shape, x.dtype), pltpu.VMEM(x.shape, x.dtype), pltpu.VMEM((4,) + x.shape, x.dtype)]
    return call(all_sum_kernel, shape(x.shape, x.dtype), (x,), [VMEM], VMEM, scratch, collective_id, 8)


def ring_sum_kernel(x_ref, out_ref, passing, direct, last, *sems):
    me, copies = lax.axis_index('tp'), Copies(sems)
    _, c, core = position(me)
    step1, step2 = ring_steps(c, core)
    first, second = me + step1 * 2, me + step2 * 2
    greet([first, second])
    chunk = out_ref.shape[0] // CHUNKS
    pieces = [pl.ds(i * chunk, chunk) for i in range(CHUNKS)]
    hops = [copies.send(x_ref.at[c + step1 + step2, p, :], passing.at[p, :], first) for p in pieces]
    sums = [copies.send(x_ref.at[c + step1], direct, first)]
    for i, p in enumerate(pieces):
        hops[i].wait()
        add_rows(passing, x_ref.at[c + step2], i * chunk, chunk)
        sums.append(copies.send(passing.at[p, :], last.at[p, :], second))
    wait_all(sums)

    def add(i, carry):
        rows = part(i, 8)
        out_ref[rows, :] = (x_ref[c, rows, :] + direct[rows, :]) + last[rows, :]
        return carry

    lax.fori_loop(0, out_ref.shape[0] // 8, add, 0)


def ring_sum(x, collective_id):
    dims = x.shape[1:]
    return call(ring_sum_kernel, shape(dims, x.dtype), (x,), [VMEM], VMEM, [pltpu.VMEM(dims, x.dtype)] * 3, collective_id, 32)


def spread_kernel(x_ref, w_ref, ring_ref, below_ref, w_out, *sems):
    me, copies = lax.axis_index('tp'), Copies(sems)
    _, c, core = position(me)
    step1, step2 = ring_steps(c, core)
    first, second = me + step1 * 2, me + step2 * 2
    up, down = line_peer(me, 1), line_peer(me, 3)
    greet([first, second, up, down])
    forth = copies.send(x_ref, ring_ref.at[c], first)
    started = [copies.send(x_ref, ring_ref.at[c], second), copies.send(x_ref, below_ref, up)]
    held = copies.local(w_ref, w_out)
    ring_ref[c] = x_ref[...]
    forth.wait()
    block = ring_ref.at[c + step1]
    wait_all(started + [copies.send(block, block, second), held])


def spread(x, w, collective_id):
    outs = (shape((4,) + x.shape, x.dtype), shape(x.shape, x.dtype), shape(w.shape, w.dtype))
    return call(spread_kernel, outs, (x, w), [VMEM, ANY], (VMEM, ANY, ANY), [], collective_id, 24)


def plane_kernel(qk_ref, v_ref, below_ref, d_ref, out_qk, out_v, far_ref, above_ref, *sems):
    me, copies = lax.axis_index('tp'), Copies(sems)
    peers = [plane_peer(me, k) for k in range(1, 8)]
    up, down = line_peer(me, 1), line_peer(me, 3)
    greet(peers + [up, down])
    mine = me % 8
    started = [copies.send(below_ref, far_ref, up), copies.send(d_ref, above_ref, down)]
    for src, dst in ((qk_ref, out_qk), (v_ref, out_v)):
        columns = part(mine, src.shape[-1])
        started += [copies.send(src.at[:, peer % 8], dst.at[:, :, columns], peer) for peer in peers]
        started.append(copies.local(src.at[:, mine], dst.at[:, :, columns]))
    wait_all(started)


def plane_exchange(qk, v, below, d, collective_id):
    outs = tuple(shape((4, a.shape[2], 8 * a.shape[3]), a.dtype) for a in (qk, v)) + (shape(below.shape, below.dtype),) * 2
    return call(plane_kernel, outs, (qk, v, below, d), [VMEM, VMEM, ANY, ANY], (ANY,) * 4, [], collective_id, 24)


def final_kernel(dqk_ref, dv_ref, wqk_ref, wv_ref, ring_ref, below_ref, above_ref, far_ref, dw_ref, o_ref, dy_ref, x_ref,
                 gx_ref, gwq_ref, gwk_ref, gwv_ref, gwo_ref,
                 dx, above, below, passing, full, buf, tile_sem, line_send, line_recv, *sems):
    me, copies = lax.axis_index('tp'), Copies(sems)
    z, c, core = position(me)
    partner = me + 1 - core * 2
    up, down = line_peer(me, 1), line_peer(me, 3)
    z_up, z_far, z_down = up // 8, line_peer(me, 2) // 8, down // 8
    ring = [ring_peer(me, k) for k in range(1, 4)]
    greet([up, down, partner] + ring)
    tiles = x_ref.shape[1] // TILE
    depth = dqk_ref.shape[1]
    line_sems = (line_send, line_recv)

    def fetch_w(j, b):
        return [pltpu.make_async_copy(wqk_ref.at[:, part(j, TILE)], buf.at[b, pl.ds(0, depth), :], tile_sem.at[0, b]),
                pltpu.make_async_copy(wv_ref.at[:, part(j, TILE)], buf.at[b, pl.ds(depth, dv_ref.shape[1]), :], tile_sem.at[1, b])]

    def fetch_x(j, b):
        return [pltpu.make_async_copy(x_ref.at[:, part(j, TILE)], buf.at[b], tile_sem.at[0, b])]

    for copy in fetch_w(0, 0):
        copy.start()
    planes, lines = [z_down, z_up, z_far], [below_ref, above_ref, far_ref]

    def slot(plane, column):
        return full.at[plane * 8 + column * 2 + core]

    rounds, shared, local = [], [], []
    for plane, block in zip(planes, lines):
        rounds += [copies.send(block, slot(plane, c), peer) for peer in ring]
    held = [(block, slot(plane, c)) for plane, block in zip(planes, lines)]
    held += [(ring_ref.at[column], slot(z, column)) for column in range(4)]
    for block, place in held:
        shared.append(copies.send(block, place, partner))
        local.append(copies.local(block, place))

    def hop(j):
        return remote(dx.at[z_far, :, part(j, TILE)], passing.at[:, part(j, TILE)], line_sems, j, up)

    def direct(j):
        return remote(dx.at[z_down, :, part(j, TILE)], above.at[:, part(j, TILE)], line_sems, tiles + j, down)

    def onward(j):
        return remote(passing.at[:, part(j, TILE)], below.at[:, part(j, TILE)], line_sems, tiles * 2 + j, up)

    def input_grad(j, carry):
        b = j % 2

        @pl.when(j + 1 < tiles)
        def _():
            for copy in fetch_w(j + 1, 1 - b):
                copy.start()

        wait_all(fetch_w(j, b))
        values = nn(dqk_ref[...], buf[b, :depth, :]) + nn(dv_ref[...], buf[b, depth:, :])
        dx[:, :, part(j, TILE)] = values.reshape(dx.shape[0], dx.shape[1], TILE)

        @pl.when(j > 0)
        def _():
            hop(j - 1).start()
            direct(j - 1).start()

        return carry

    lax.fori_loop(0, tiles, input_grad, 0)
    for copy in fetch_x(0, 0):
        copy.start()

    def weight_grad(j, carry):
        b = j % 2

        @pl.when(j + 1 < tiles)
        def _():
            for copy in fetch_x(j + 1, 1 - b):
                copy.start()

        wait_all(fetch_x(j, b))

        @pl.when(j == 0)
        def _():
            hop(tiles - 1).start()
            direct(tiles - 1).start()

        hop(j).wait()
        passing[:, part(j, TILE)] = passing[:, part(j, TILE)] + dx[z_up, :, part(j, TILE)]
        values = nn(dw_ref[...], buf[b]).T
        for i, ref in enumerate((gwq_ref, gwk_ref, gwv_ref)):
            ref[part(j, TILE), :] = values[:, i * HEAD_SIZE:(i + 1) * HEAD_SIZE].astype(ref.dtype)
        onward(j).start()
        return carry

    lax.fori_loop(0, tiles, weight_grad, 0)
    for i, copy in enumerate(rounds):
        copy.wait()
        block = slot(planes[i // 3], (c + 3 - i % 3) % 4)
        shared.append(copies.send(block, block, partner))

    def finish(j, carry):
        direct(j).wait()
        onward(j).wait()
        tile = part(j, TILE)
        total = (dx[z, :, tile] + above[:, tile]) + below[:, tile]
        gx_ref[:, tile] = (total + dy_ref[:, tile].astype(jnp.float32)).astype(gx_ref.dtype)
        return carry

    lax.fori_loop(0, tiles, finish, 0)
    wait_all(local + shared)

    def out_grad(j, carry):
        d = full[:, :, part(j, TILE)]
        gwo_ref[:, part(j, TILE)] = nn(o_ref[...], d.reshape(o_ref.shape[1], TILE)).astype(gwo_ref.dtype)
        return carry

    lax.fori_loop(0, tiles, out_grad, 0)


def final(dqk, dv, wqk, wv, d_ring, d_below, d_above, d_far, dw_rows, o_rows, dy, x_full, collective_id):
    rows, model_dim = d_far.shape
    seq_len = x_full.shape[0]
    bf16, f32 = d_far.dtype, jnp.float32
    block = pltpu.VMEM((rows, model_dim), f32)
    scratch = [pltpu.VMEM((dqk.shape[0] // rows, rows, model_dim), f32), block, block, block,
               pltpu.VMEM((seq_len // rows, rows, model_dim), bf16), pltpu.VMEM((2, seq_len, TILE), bf16), pltpu.SemaphoreType.DMA((2, 2)),
               pltpu.SemaphoreType.DMA((SEMAPHORES,)), pltpu.SemaphoreType.DMA((SEMAPHORES,))]
    outs = (shape(dy.shape, bf16),) + (shape((model_dim, HEAD_SIZE), bf16),) * 3 + (shape((o_rows.shape[0], model_dim), bf16),)
    return call(final_kernel, outs, (dqk, dv, wqk, wv, d_ring, d_below, d_above, d_far, dw_rows, o_rows, dy, x_full),
                [VMEM] * 2 + [ANY] * 6 + [VMEM] * 3 + [ANY], (VMEM,) * 5,
                scratch, collective_id, 60)


def gather_kernel(x_ref, wq_ref, wk_ref, wv_ref, wo_ref, out_ref, q_ref, k_ref, v_ref, col_ref, wqk_rows, wv_rows,
                  full, weights, rows_scr, qk_scr, total, *sems):
    me, copies = lax.axis_index('tp'), Copies(sems)
    z, c, core = position(me)
    partner = me + 1 - core * 2
    step1, step2 = ring_steps(c, core)
    first, second = me + step1 * 2, me + step2 * 2
    up, far, down = [line_peer(me, k) for k in range(1, 4)]
    planes = [z, down // 8, up // 8, far // 8]
    direct, corner = (0, 1, 3, 5), (2, 4, 6, 7)

    def slot(plane, column):
        return full.at[plane * 8 + column * 2 + core]

    own = copies.local(x_ref, slot(z, c))
    loads = [copies.local(ref, weights.at[:, pl.ds(i * HEAD_SIZE, HEAD_SIZE)]) for i, ref in enumerate((wq_ref, wk_ref, wv_ref))]
    greet([up, down, first, second, partner])
    own.wait()
    line = {i: copies.send(slot(z, c), slot(z, c), peer) for i, peer in ((1, up), (2, down))}
    to_first, to_second, to_partner, stores = {}, {}, {}, []

    def forward(s, column, index, slot_of):
        block = slot(planes[s], column)
        if index is not None:
            to_second[index] = copies.send(block, block, second)
        to_partner[slot_of] = copies.send(block, block, partner)

    def pass_on(s):
        block = slot(planes[s], c)
        to_first[s] = copies.send(block, block, first)
        forward(s, c, direct[s], s)

    def from_line(s):
        line[s].wait()
        pass_on(s)

    head, head_line, head_partner = (lambda plane: col_ref.at[plane * 2 + core]), {}, []

    def head_from_line(s):
        head_line[s].wait()
        block = head(planes[s])
        if s == 1:
            head_line[3] = copies.send(block, block, up)
        head_partner.append(copies.send(block, block, partner))

    def from_first(s):
        to_first[s].wait()
        forward(s, c + step1, corner[s], 4 + s)

    def from_second(i):
        to_second[i].wait()
        if i in direct:
            forward(direct.index(i), c + step2, None, 8 + i)
        else:
            forward(corner.index(i), c + step2 + step1, None, 8 + i)

    def multiply(s, column, slot_of):
        to_partner[slot_of].wait()
        pair = planes[s] * 4 + column
        blocks = pl.ds(pair * 2, 2)
        stores.append(copies.local(full.at[blocks], out_ref.at[blocks]))
        rows = part(pair, total.shape[0])
        total[...] = jnp.zeros_like(total)

        def chunk(i, carry):
            depth = part(i, DEPTH)
            a = full[blocks, :, depth].reshape(rows.size, DEPTH)
            total[...] += nn(a, weights[depth, :])
            return carry

        lax.fori_loop(0, weights.shape[0] // DEPTH, chunk, 0)
        qk_scr[rows, :] = total[:, :2 * HEAD_SIZE]
        v_ref[rows, :] = total[:, 2 * HEAD_SIZE:].astype(v_ref.dtype)

    def multiply_own(s):
        multiply(s, c, s)

    def multiply_sides(s):
        multiply(s, c + step1, 8 + direct[s])
        multiply(s, c + step2, 4 + s)

    def multiply_corner(s):
        multiply(s, c + step1 + step2, 8 + corner[s])

    pass_on(0)
    from_line(1)
    line[3] = copies.send(slot(planes[1], c), slot(planes[1], c), up)
    own_head = copies.local(wo_ref, head(z))
    head_line[1] = copies.send(wo_ref, head(z), up)
    head_line[2] = copies.send(wo_ref, head(z), down)
    head_partner.append(copies.send(wo_ref, head(z), partner))
    from_first(0)
    wait_all(loads)
    multiply_own(0)

    def transpose(i, carry):
        rows_scr[:, part(i, TILE)] = weights[part(i, TILE), :].T
        return carry

    lax.fori_loop(0, weights.shape[0] // TILE, transpose, 0)
    from_second(0)
    from_line(2)
    from_first(1)
    multiply_own(1)
    from_second(1)
    from_first(2)
    from_line(3)
    stores.append(copies.local(rows_scr.at[pl.ds(0, 2 * HEAD_SIZE), :], wqk_rows))
    stores.append(copies.local(rows_scr.at[pl.ds(2 * HEAD_SIZE, HEAD_SIZE), :], wv_rows))
    multiply_own(2)
    from_second(2)
    head_from_line(1)
    multiply_sides(0)
    from_first(3)
    multiply_own(3)
    from_second(3)
    multiply_sides(1)
    from_second(4)
    multiply_corner(0)
    from_second(5)
    multiply_sides(2)
    head_from_line(2)
    from_second(6)
    multiply_sides(3)
    multiply_corner(1)
    from_second(7)
    multiply_corner(2)
    multiply_corner(3)

    def turn(i, carry):
        values = qk_scr[part(i, TILE), :].T
        q_ref[:, part(i, TILE)] = values[:HEAD_SIZE]
        k_ref[:, part(i, TILE)] = values[HEAD_SIZE:]
        return carry

    lax.fori_loop(0, qk_scr.shape[0] // TILE, turn, 0)
    head_from_line(3)
    wait_all(stores + [own_head] + head_partner)


def gather(x, wq, wk, wv, wo, devices, collective_id):
    rows, model_dim = x.shape
    f32 = jnp.float32
    head = (devices * rows, HEAD_SIZE)
    outs = (shape((devices, rows, model_dim), x.dtype), shape(head[::-1], f32), shape(head[::-1], f32), shape(head, x.dtype),
            shape((8,) + wo.shape, wo.dtype), shape((2 * HEAD_SIZE, model_dim), x.dtype), shape((HEAD_SIZE, model_dim), x.dtype))
    width = 3 * HEAD_SIZE
    scratch = [pltpu.VMEM((devices, rows, model_dim), x.dtype), pltpu.VMEM((model_dim, width), x.dtype),
               pltpu.VMEM((width, model_dim), x.dtype), pltpu.VMEM((devices * rows, 2 * HEAD_SIZE), f32), pltpu.VMEM((2 * rows, width), f32)]
    return call(gather_kernel, outs, (x, wq, wk, wv, wo), [ANY] * 5, (ANY, VMEM, VMEM, VMEM, ANY, ANY, ANY), scratch, collective_id, 62)


def nt(a, b):
    return lax.dot_general(a, b, (((1,), (1,)), ((), ())), preferred_element_type=jnp.float32)


def tn(a, b):
    return lax.dot_general(a, b, (((0,), (0,)), ((), ())), preferred_element_type=jnp.float32)


def nn(a, b):
    return lax.dot_general(a, b, (((1,), (0,)), ((), ())), preferred_element_type=jnp.float32)


def fold_rows(values, op):
    return op(values.reshape(values.shape[0] // 8, 8, values.shape[1]), axis=0)


def block_rows(j):
    return pl.ds(pl.multiple_of(j * BLOCK, BLOCK), BLOCK)


def diagonal_mask():
    keys = lax.broadcasted_iota(jnp.int32, (BLOCK, BLOCK), 0)
    queries = lax.broadcasted_iota(jnp.int32, (BLOCK, BLOCK), 1)
    return keys <= queries


def attention_kernel(q_ref, k_ref, v_ref, o_ref, ot_ref, max_ref, inv_ref, s_scr, acc_scr):
    i = pl.program_id(0)
    q_blk = q_ref[...]

    def score(j, top):
        s = tn(k_ref[:, block_rows(j)], q_blk) * (ATTN_SCALE * LOG2E)
        s_scr[block_rows(j), :] = s
        return jnp.maximum(top, fold_rows(s, jnp.max))

    s = jnp.where(diagonal_mask(), tn(k_ref[:, block_rows(i)], q_blk) * (ATTN_SCALE * LOG2E), -1e30)
    s_scr[block_rows(i), :] = s
    top = lax.fori_loop(0, i, score, fold_rows(s, jnp.max))
    top = jnp.max(top, axis=0, keepdims=True)

    def weigh(j, total):
        p = jnp.exp2(s_scr[block_rows(j), :] - top)
        s_scr[block_rows(j), :] = p
        return total + fold_rows(p, jnp.sum)

    total = lax.fori_loop(0, i + 1, weigh, jnp.zeros((8, BLOCK), jnp.float32))
    inv = 1.0 / jnp.sum(total, axis=0, keepdims=True)
    max_ref[...] = top
    inv_ref[...] = inv
    acc_scr[...] = jnp.zeros_like(acc_scr)

    def gather(j, carry):
        p = (s_scr[block_rows(j), :] * inv).astype(jnp.bfloat16)
        acc_scr[...] += tn(v_ref[block_rows(j), :], p)
        return carry

    lax.fori_loop(0, i + 1, gather, 0)
    o_ref[...] = acc_scr[...].T.astype(jnp.bfloat16)
    ot_ref[...] = acc_scr[...].astype(jnp.bfloat16)


def attention(q, k, v):
    seq_len = v.shape[0]
    steps = seq_len // BLOCK
    rows = pl.BlockSpec((BLOCK, HEAD_SIZE), lambda i: (i, 0))
    whole = pl.BlockSpec((seq_len, HEAD_SIZE), lambda i: (0, 0))
    line = pl.BlockSpec((1, BLOCK), lambda i: (0, i))
    columns = pl.BlockSpec((HEAD_SIZE, BLOCK), lambda i: (0, i))
    wide = pl.BlockSpec((HEAD_SIZE, seq_len), lambda i: (0, 0))
    return pl.pallas_call(
        attention_kernel,
        grid=(steps,),
        out_shape=(jax.ShapeDtypeStruct((seq_len, HEAD_SIZE), jnp.bfloat16),
                   jax.ShapeDtypeStruct((HEAD_SIZE, seq_len), jnp.bfloat16),
                   jax.ShapeDtypeStruct((1, seq_len), jnp.float32),
                   jax.ShapeDtypeStruct((1, seq_len), jnp.float32)),
        in_specs=[columns, wide, whole], out_specs=(rows, columns, line, line),
        scratch_shapes=[pltpu.VMEM((seq_len, BLOCK), jnp.float32), pltpu.VMEM((HEAD_SIZE, BLOCK), jnp.float32)],
        compiler_params=pltpu.CompilerParams(dimension_semantics=("arbitrary",), vmem_limit_bytes=40 << 20),
        cost_estimate=pl.CostEstimate(flops=8 * seq_len * seq_len * HEAD_SIZE, bytes_accessed=8 * seq_len * HEAD_SIZE, transcendentals=0),
    )(q, k, v)


def attention_grad_kernel(q_ref, k_ref, v_ref, do_ref, max_ref, inv_ref, dq_ref, dk_ref, dv_ref, dvt_ref, p_scr, dp_scr, dq_scr, dk_scr, dv_scr):
    i = pl.program_id(0)
    q_blk, do_blk = q_ref[...], do_ref[...]
    top, inv = max_ref[...], inv_ref[...]

    @pl.when(i == 0)
    def _():
        dk_scr[...] = jnp.zeros_like(dk_scr)
        dv_scr[...] = jnp.zeros_like(dv_scr)

    def scores(j, mask, delta):
        rows = block_rows(j)
        s = tn(k_ref[:, rows], q_blk) * (ATTN_SCALE * LOG2E)
        if mask is not None:
            s = jnp.where(mask, s, -1e30)
        p = jnp.exp2(s - top) * inv
        dp = nt(v_ref[rows, :], do_blk)
        p_scr[rows, :] = p
        dp_scr[rows, :] = dp
        dv_scr[rows, :] += nn(p.astype(jnp.bfloat16), do_blk)
        return delta + fold_rows(p * dp, jnp.sum)

    delta = scores(i, diagonal_mask(), jnp.zeros((8, BLOCK), jnp.float32))
    delta = lax.fori_loop(0, i, lambda j, d: scores(j, None, d), delta)
    delta = jnp.sum(delta, axis=0, keepdims=True)
    dq_scr[...] = jnp.zeros_like(dq_scr)

    def grads(j, carry):
        rows = block_rows(j)
        ds = (p_scr[rows, :] * (dp_scr[rows, :] - delta) * ATTN_SCALE).astype(jnp.bfloat16)
        dk_scr[:, rows] += nt(q_blk, ds)
        dq_scr[...] += nn(k_ref[:, rows], ds)
        return carry

    lax.fori_loop(0, i + 1, grads, 0)
    dq_ref[...] = dq_scr[...]

    @pl.when(i == pl.num_programs(0) - 1)
    def _():
        dk_ref[...] = dk_scr[...]
        dv_ref[...] = dv_scr[...].astype(jnp.bfloat16)

        def turn(j, carry):
            dvt_ref[:, block_rows(j)] = dv_scr[block_rows(j), :].T.astype(jnp.bfloat16)
            return carry

        lax.fori_loop(0, pl.num_programs(0), turn, 0)


def attention_grad(q, k, v, do, top, inv):
    seq_len = v.shape[0]
    steps = seq_len // BLOCK
    rows = pl.BlockSpec((BLOCK, HEAD_SIZE), lambda i: (i, 0))
    whole = pl.BlockSpec((seq_len, HEAD_SIZE), lambda i: (0, 0))
    line = pl.BlockSpec((1, BLOCK), lambda i: (0, i))
    columns = pl.BlockSpec((HEAD_SIZE, BLOCK), lambda i: (0, i))
    wide = pl.BlockSpec((HEAD_SIZE, seq_len), lambda i: (0, 0))
    full, turned = (seq_len, HEAD_SIZE), (HEAD_SIZE, seq_len)
    return pl.pallas_call(
        attention_grad_kernel,
        grid=(steps,),
        out_shape=(shape(turned, jnp.float32), shape(turned, jnp.float32), shape(full, jnp.bfloat16), shape(turned, jnp.bfloat16)),
        in_specs=[columns, wide, whole, rows, line, line], out_specs=(columns, wide, whole, wide),
        scratch_shapes=[pltpu.VMEM((seq_len, BLOCK), jnp.float32), pltpu.VMEM((seq_len, BLOCK), jnp.float32),
                        pltpu.VMEM((HEAD_SIZE, BLOCK), jnp.float32), pltpu.VMEM(turned, jnp.float32), pltpu.VMEM(full, jnp.float32)],
        compiler_params=pltpu.CompilerParams(dimension_semantics=("arbitrary",), vmem_limit_bytes=48 << 20),
        cost_estimate=pl.CostEstimate(flops=20 * seq_len * seq_len * HEAD_SIZE, bytes_accessed=20 * seq_len * HEAD_SIZE, transcendentals=0),
    )(q, k, v, do, top, inv)


COLUMN_GROUPS = [[z * 8 + c * 2 + core for z in range(4) for core in range(2)] for c in range(4)]
PLANE_GROUPS = [[z * 8 + p for p in range(8)] for z in range(4)]


def lane_rows(values):
    return values.reshape(-1, 128)


def local_block(x_loc, wq_loc, wk_loc, wv_loc, wo_loc, gq_loc, gk_loc, g_attn, dy_loc):
    x_loc, dy_loc = x_loc[0], dy_loc[0]
    rows, model_dim = x_loc.shape
    bf16, f32 = jnp.bfloat16, jnp.float32
    x_blocks, q_raw, k_raw, v_head, wo_blocks, wqk_rows, wv_rows = gather(x_loc, wq_loc, wk_loc, wv_loc, wo_loc, 32, 9)
    wo_col = wo_blocks.reshape(8 * HEAD_SIZE, model_dim)
    x_full = x_blocks.reshape(32 * rows, model_dim)
    seq_len = x_full.shape[0]
    wv_plane = lax.all_gather(wv_rows, 'tp', axis=0, tiled=True, axis_index_groups=PLANE_GROUPS)
    cos_t, sin_t = rope_tables(seq_len)
    stats = jnp.concatenate([lane_rows(jnp.sum(q_raw * q_raw, axis=0)), lane_rows(jnp.sum(k_raw * k_raw, axis=0))])
    sq_sums = all_sum(stats, 1).reshape(2, seq_len)
    inv_rms = lax.rsqrt(sq_sums / model_dim + NORM_EPS)[:, None, :]
    q_unit = q_raw * inv_rms[0]
    k_unit = k_raw * inv_rms[1]
    gq_f, gk_f = gq_loc.astype(f32)[:, None], gk_loc.astype(f32)[:, None]
    q_rot = rotate(q_unit * gq_f, cos_t, sin_t).astype(bf16)
    k_rot = rotate(k_unit * gk_f, cos_t, sin_t).astype(bf16)
    o_head, o_rows, top, inv = attention(q_rot, k_rot, v_head)

    o_col = exchange(
        o_head.reshape(4, 4, 2, rows, HEAD_SIZE), (4, rows, 8 * HEAD_SIZE), column_peer, 8,
        lambda ref, d: ref.at[d // 8, :, d % 2],
        lambda ref, d: ref.at[:, :, part(member_of(d), HEAD_SIZE)], 2)
    a_part = nn(o_col.reshape(4 * rows, 8 * HEAD_SIZE), wo_col)
    attn_loc = ring_sum(a_part.reshape(4, rows, model_dim), 3)

    post_rms = lax.rsqrt(jnp.mean(attn_loc * attn_loc, axis=-1, keepdims=True) + NORM_EPS)
    normed = attn_loc * post_rms
    ga_f = g_attn.astype(f32)
    dy_f = dy_loc.astype(f32)
    y_loc = (x_loc.astype(f32) + normed * ga_f).astype(bf16)
    ga_part = jnp.sum(dy_f * normed, axis=0)
    g_normed = dy_f * ga_f
    d_attn = (post_rms * (g_normed - normed * jnp.mean(g_normed * normed, axis=-1, keepdims=True))).astype(bf16)

    d_ring, d_below, wqk_after = spread(d_attn, wqk_rows, 4)
    wqk_plane = lax.all_gather(wqk_after, 'tp', axis=0, tiled=True, axis_index_groups=PLANE_GROUPS)
    d_col = nt(d_ring.reshape(4 * rows, model_dim), wo_col).astype(bf16)
    d_head = exchange(
        d_col.reshape(4, rows, 8 * HEAD_SIZE), (4, 4, 2, rows, HEAD_SIZE), column_peer, 8,
        lambda ref, d: ref.at[:, :, part(member_of(d), HEAD_SIZE)],
        lambda ref, d: ref.at[d // 8, :, d % 2], 5).reshape(seq_len, HEAD_SIZE)

    dq_rot, dk_rot, d_value, d_value_rows = attention_grad(q_rot, k_rot, v_head, d_head, top, inv)
    dq_hat = rotate_back(dq_rot, cos_t, sin_t)
    dk_hat = rotate_back(dk_rot, cos_t, sin_t)
    grad_gq = jnp.sum(dq_hat * q_unit, axis=1)
    grad_gk = jnp.sum(dk_hat * k_unit, axis=1)
    dq_unit = dq_hat * gq_f
    dk_unit = dk_hat * gk_f
    sums = jnp.concatenate([lane_rows(jnp.sum(dq_unit * q_unit, axis=0)), lane_rows(jnp.sum(dk_unit * k_unit, axis=0)), lane_rows(ga_part)])
    sums = all_sum(sums, 6)
    dots_rows = 2 * seq_len // 128
    unit_dots = sums[:dots_rows].reshape(2, seq_len)[:, None, :] / model_dim
    grad_ga = sums[dots_rows:].reshape(model_dim)
    dq_raw = (inv_rms[0] * (dq_unit - q_unit * unit_dots[0])).astype(bf16)
    dk_raw = (inv_rms[1] * (dk_unit - k_unit * unit_dots[1])).astype(bf16)
    dqk_rows = jnp.concatenate([dq_raw, dk_raw], axis=0)
    d_qk = dqk_rows.T
    dw_rows = jnp.concatenate([dqk_rows, d_value_rows], axis=0)

    dqk_plane, dv_plane, d_far, d_above = plane_exchange(
        d_qk.reshape(4, 8, rows, 2 * HEAD_SIZE), d_value.reshape(4, 8, rows, HEAD_SIZE), d_below, d_attn, 7)
    grad_x, grad_wq, grad_wk, grad_wv, grad_wo = final(
        dqk_plane.reshape(4 * rows, 16 * HEAD_SIZE), dv_plane.reshape(4 * rows, 8 * HEAD_SIZE), wqk_plane, wv_plane,
        d_ring, d_below, d_above, d_far, dw_rows, o_rows, dy_loc, x_full, 8)
    return (y_loc[None], grad_x[None], grad_wq, grad_wk, grad_wv, grad_wo,
            grad_gq.astype(bf16), grad_gk.astype(bf16), grad_ga.astype(bf16))


def solution(mesh):
    act_spec = P(None, 'tp', None)
    col_spec = P(None, 'tp')
    row_spec = P('tp', None)
    vec_spec = P('tp')
    in_specs = (act_spec, col_spec, col_spec, col_spec, row_spec, vec_spec, vec_spec, P(), act_spec)
    out_specs = (act_spec, act_spec, col_spec, col_spec, col_spec, row_spec, vec_spec, vec_spec, P())
    return jax.shard_map(local_block, mesh=mesh, in_specs=in_specs, out_specs=out_specs, check_vma=False)
```

```python
import functools

import jax
import jax.numpy as jnp
from jax import lax
from jax.experimental import pallas as pl
from jax.experimental.pallas import tpu as pltpu
from jax.sharding import PartitionSpec as P

HEAD_SIZE = 128
ROPE_THETA = 500000.0
NORM_EPS = 1e-6
LOG2E = 1.4426950408889634
ATTN_SCALE = HEAD_SIZE ** -0.5
MESH = pl.DeviceIdType.MESH
VMEM = pl.BlockSpec(memory_space=pltpu.VMEM)
BLOCK = 512


def rope_tables(seq_len):
    half_dim = HEAD_SIZE // 2
    inv_freq = 1.0 / (ROPE_THETA ** (jnp.arange(half_dim, dtype=jnp.float32) / half_dim))
    angles = inv_freq[:, None] * jnp.arange(seq_len, dtype=jnp.float32)[None, :]
    return jnp.cos(angles), jnp.sin(angles)


def rotate(values, cos_t, sin_t):
    lower_half, upper_half = jnp.split(values, 2, axis=0)
    return jnp.concatenate([lower_half * cos_t - upper_half * sin_t, upper_half * cos_t + lower_half * sin_t], axis=0)


def rotate_back(values, cos_t, sin_t):
    return rotate(values, cos_t, -sin_t)


SEMAPHORES = 72
DEPTH = 1024
CHUNKS = 4
TILE = 512
ANY = pl.BlockSpec(memory_space=pl.ANY)


def position(d):
    return d // 8, d // 2 % 4, d % 2


def member_of(d):
    z, _, core = position(d)
    return z * 2 + core


def column_peer(me, k):
    member = (member_of(me) + k) % 8
    return member // 2 * 8 + position(me)[1] * 2 + member % 2


def plane_peer(me, k):
    return me - me % 8 + (me + k) % 8


def line_peer(me, k):
    return (me + k * 8) % 32


def ring_steps(c, core):
    step_x, step_y = 1 - c % 2 * 2, 2 - c // 2 * 4
    step1 = step_x * (1 - core) + step_y * core
    return step1, step_x + step_y - step1


def greet(peers):
    barrier = pltpu.get_barrier_semaphore()
    for peer in peers:
        pl.semaphore_signal(barrier, inc=1, device_id=(peer,), device_id_type=MESH)
    pl.semaphore_wait(barrier, len(peers))


def remote(src, dst, sems, slot, peer):
    return pltpu.make_async_remote_copy(
        src_ref=src, dst_ref=dst, send_sem=sems[0].at[slot], recv_sem=sems[1].at[slot], device_id=(peer,), device_id_type=MESH)


class Copies:
    def __init__(self, sems):
        self.sems, self.used = sems, 0

    def send(self, src, dst, peer):
        copy = remote(src, dst, self.sems, self.used, peer)
        copy.start()
        self.used += 1
        return copy

    def local(self, src, dst):
        copy = pltpu.make_async_copy(src, dst, self.sems[2].at[self.used])
        copy.start()
        self.used += 1
        return copy


def wait_all(copies):
    for copy in copies:
        copy.wait()


def call(kernel, out_shape, operands, in_specs, out_specs, scratch, collective_id, mib):
    return pl.pallas_call(
        kernel, out_shape=out_shape, in_specs=in_specs, out_specs=out_specs,
        scratch_shapes=list(scratch) + [pltpu.SemaphoreType.DMA((SEMAPHORES,))] * 3,
        compiler_params=pltpu.CompilerParams(collective_id=collective_id, has_side_effects=True, vmem_limit_bytes=mib << 20),
    )(*operands)


def shape(dims, dtype):
    return jax.ShapeDtypeStruct(tuple(dims), dtype)


def part(index, size):
    return pl.ds(pl.multiple_of(index * size, size), size)


def add_rows(ref, other, start, count):
    def add(i, carry):
        rows = part(start // 8 + i, 8)
        ref[rows, :] = ref[rows, :] + other[rows, :]
        return carry

    lax.fori_loop(0, count // 8, add, 0)


def exchange_kernel(peer_of, count, source, target, x_ref, out_ref, *sems):
    me, copies = lax.axis_index('tp'), Copies(sems)
    peers = [peer_of(me, k) for k in range(1, count)]
    greet(peers)
    started = [copies.send(source(x_ref, peer), target(out_ref, me), peer) for peer in peers]
    target(out_ref, me)[...] = source(x_ref, me)[...]
    wait_all(started)


def exchange(x, out_shape, peer_of, count, source, target, collective_id):
    kernel = functools.partial(exchange_kernel, peer_of, count, source, target)
    return call(kernel, shape(out_shape, x.dtype), (x,), [VMEM], VMEM, [], collective_id, 24)


def all_sum_kernel(x_ref, out_ref, plane, middle, line, *sems):
    me, copies = lax.axis_index('tp'), Copies(sems)
    z, mine = me // 8, me % 8
    plane_peers = [plane_peer(me, k) for k in range(1, 8)]
    line_peers = [line_peer(me, k) for k in range(1, 4)]
    greet(plane_peers + line_peers)
    started = [copies.send(x_ref, plane.at[mine], peer) for peer in plane_peers]
    plane[mine] = x_ref[...]
    wait_all(started)
    total = plane[0]
    for k in range(1, 8):
        total = total + plane[k]
    middle[...] = total
    line[z] = total
    wait_all([copies.send(middle, line.at[z], peer) for peer in line_peers])
    out_ref[...] = (line[0] + line[1]) + (line[2] + line[3])


def all_sum(x, collective_id):
    scratch = [pltpu.VMEM((8,) + x.shape, x.dtype), pltpu.VMEM(x.shape, x.dtype), pltpu.VMEM((4,) + x.shape, x.dtype)]
    return call(all_sum_kernel, shape(x.shape, x.dtype), (x,), [VMEM], VMEM, scratch, collective_id, 8)


def ring_sum_kernel(x_ref, out_ref, passing, direct, last, *sems):
    me, copies = lax.axis_index('tp'), Copies(sems)
    _, c, core = position(me)
    step1, step2 = ring_steps(c, core)
    first, second = me + step1 * 2, me + step2 * 2
    greet([first, second])
    chunk = out_ref.shape[0] // CHUNKS
    pieces = [pl.ds(i * chunk, chunk) for i in range(CHUNKS)]
    hops = [copies.send(x_ref.at[c + step1 + step2, p, :], passing.at[p, :], first) for p in pieces]
    sums = [copies.send(x_ref.at[c + step1], direct, first)]
    for i, p in enumerate(pieces):
        hops[i].wait()
        add_rows(passing, x_ref.at[c + step2], i * chunk, chunk)
        sums.append(copies.send(passing.at[p, :], last.at[p, :], second))
    wait_all(sums)

    def add(i, carry):
        rows = part(i, 8)
        out_ref[rows, :] = (x_ref[c, rows, :] + direct[rows, :]) + last[rows, :]
        return carry

    lax.fori_loop(0, out_ref.shape[0] // 8, add, 0)


def ring_sum(x, collective_id):
    dims = x.shape[1:]
    return call(ring_sum_kernel, shape(dims, x.dtype), (x,), [VMEM], VMEM, [pltpu.VMEM(dims, x.dtype)] * 3, collective_id, 32)


def spread_kernel(x_ref, w_ref, ring_ref, below_ref, above_ref, w_out, *sems):
    me, copies = lax.axis_index('tp'), Copies(sems)
    _, c, core = position(me)
    step1, step2 = ring_steps(c, core)
    first, second = me + step1 * 2, me + step2 * 2
    up, down = line_peer(me, 1), line_peer(me, 3)
    greet([first, second, up, down])
    forth = copies.send(x_ref, ring_ref.at[c], first)
    started = [copies.send(x_ref, ring_ref.at[c], second), copies.send(x_ref, below_ref, up),
               copies.send(x_ref.at[pl.ds(0, above_ref.shape[0]), :], above_ref, down)]
    held = copies.local(w_ref, w_out)
    ring_ref[c] = x_ref[...]
    forth.wait()
    block = ring_ref.at[c + step1]
    wait_all(started + [copies.send(block, block, second), held])


def spread(x, w, collective_id):
    half = shape((x.shape[0] // 2, x.shape[1]), x.dtype)
    outs = (shape((4,) + x.shape, x.dtype), shape(x.shape, x.dtype), half, shape(w.shape, w.dtype))
    return call(spread_kernel, outs, (x, w), [VMEM, ANY], (VMEM, ANY, ANY, ANY), [], collective_id, 24)


def plane_kernel(qk_ref, v_ref, below_ref, d_ref, out_qk, out_v, far_ref, above_ref, *sems):
    me, copies = lax.axis_index('tp'), Copies(sems)
    peers = [plane_peer(me, k) for k in range(1, 8)]
    up, down = line_peer(me, 1), line_peer(me, 3)
    greet(peers + [up, down])
    mine = me % 8
    started = [copies.send(below_ref, far_ref, up), copies.send(d_ref.at[pl.ds(above_ref.shape[0], above_ref.shape[0]), :], above_ref, down)]
    for src, dst in ((qk_ref, out_qk), (v_ref, out_v)):
        columns = part(mine, src.shape[-1])
        started += [copies.send(src.at[:, peer % 8], dst.at[:, :, columns], peer) for peer in peers]
        started.append(copies.local(src.at[:, mine], dst.at[:, :, columns]))
    wait_all(started)


def plane_exchange(qk, v, below, d, collective_id):
    outs = tuple(shape((4, a.shape[2], 8 * a.shape[3]), a.dtype) for a in (qk, v)) + (
        shape(below.shape, below.dtype), shape((d.shape[0] // 2, d.shape[1]), d.dtype))
    return call(plane_kernel, outs, (qk, v, below, d), [VMEM, VMEM, ANY, ANY], (ANY,) * 4, [], collective_id, 62)


def final_kernel(dqk_ref, dv_ref, wqk_ref, wv_ref, ring_ref, below_ref, top_ref, low_ref, far_ref, dwqk_ref, dwv_ref, o_ref, dy_ref, x_ref,
                 gx_ref, gwq_ref, gwk_ref, gwv_ref, gwo_ref,
                 dx, above, below, passing, full, buf, tile_sem, line_send, line_recv, *sems):
    me, copies = lax.axis_index('tp'), Copies(sems)
    z, c, core = position(me)
    partner = me + 1 - core * 2
    up, down = line_peer(me, 1), line_peer(me, 3)
    z_up, z_far, z_down = up // 8, line_peer(me, 2) // 8, down // 8
    step1, step2 = ring_steps(c, core)
    first, second = me + step1 * 2, me + step2 * 2
    greet([up, down, partner, first, second])
    tiles = x_ref.shape[1] // TILE
    depth = dqk_ref.shape[1]
    line_sems = (line_send, line_recv)

    def fetch_w(j, b):
        return [pltpu.make_async_copy(wqk_ref.at[:, part(j, TILE)], buf.at[b, pl.ds(0, depth), :], tile_sem.at[0, b]),
                pltpu.make_async_copy(wv_ref.at[:, part(j, TILE)], buf.at[b, pl.ds(depth, dv_ref.shape[1]), :], tile_sem.at[1, b])]

    def fetch_x(j, b):
        return [pltpu.make_async_copy(x_ref.at[:, part(j, TILE)], buf.at[b], tile_sem.at[0, b])]

    for copy in fetch_w(0, 0):
        copy.start()
    half = top_ref.shape[0]
    whole = pl.ds(0, 2 * half)
    pieces = [(z_down, whole, below_ref), (z_up, pl.ds(0, half), top_ref), (z_up, pl.ds(half, half), low_ref), (z_far, whole, far_ref)]

    def spot(plane, column, rows):
        return full.at[plane * 8 + column * 2 + core, rows, :]

    to_first = [copies.send(block, spot(plane, c, rows), first) for plane, rows, block in pieces]
    to_second = [copies.send(block, spot(plane, c, rows), second) for plane, rows, block in pieces]
    to_corner, shared, local = [], [], []
    held = [(block, spot(plane, c, rows)) for plane, rows, block in pieces]
    held += [(ring_ref.at[column], spot(z, column, whole)) for column in range(4)]
    for block, place in held:
        shared.append(copies.send(block, place, partner))
        local.append(copies.local(block, place))

    def pass_on(copy, plane, column, rows):
        copy.wait()
        block = spot(plane, column, rows)
        shared.append(copies.send(block, block, partner))
        return block

    def hop(j):
        return remote(dx.at[z_far, :, part(j, TILE)], passing.at[:, part(j, TILE)], line_sems, j, up)

    def direct(j):
        return remote(dx.at[z_down, :, part(j, TILE)], above.at[:, part(j, TILE)], line_sems, tiles + j, down)

    def onward(j):
        return remote(passing.at[:, part(j, TILE)], below.at[:, part(j, TILE)], line_sems, tiles * 2 + j, up)

    def input_grad(j, carry):
        b = j % 2

        @pl.when(j + 1 < tiles)
        def _():
            for copy in fetch_w(j + 1, 1 - b):
                copy.start()

        wait_all(fetch_w(j, b))
        values = nn(dqk_ref[...], buf[b, :depth, :]) + nn(dv_ref[...], buf[b, depth:, :])
        dx[:, :, part(j, TILE)] = values.reshape(dx.shape[0], dx.shape[1], TILE)

        @pl.when(j > 0)
        def _():
            hop(j - 1).start()
            direct(j - 1).start()

        return carry

    lax.fori_loop(0, tiles, input_grad, 0)
    for copy in fetch_x(0, 0):
        copy.start()

    def weight_grad(j, carry):
        b = j % 2

        @pl.when(j + 1 < tiles)
        def _():
            for copy in fetch_x(j + 1, 1 - b):
                copy.start()

        wait_all(fetch_x(j, b))

        @pl.when(j == 0)
        def _():
            hop(tiles - 1).start()
            direct(tiles - 1).start()

        hop(j).wait()
        passing[:, part(j, TILE)] = passing[:, part(j, TILE)] + dx[z_up, :, part(j, TILE)]
        values = nn(dwqk_ref[...], buf[b]).T
        gwq_ref[part(j, TILE), :] = values[:, :HEAD_SIZE].astype(gwq_ref.dtype)
        gwk_ref[part(j, TILE), :] = values[:, HEAD_SIZE:].astype(gwk_ref.dtype)
        gwv_ref[part(j, TILE), :] = nn(dwv_ref[...], buf[b]).T.astype(gwv_ref.dtype)
        onward(j).start()
        return carry

    lax.fori_loop(0, tiles, weight_grad, 0)
    for copy, (plane, rows, _) in zip(to_first, pieces):
        block = pass_on(copy, plane, c + step1, rows)
        to_corner.append(copies.send(block, block, second))
    for column, arrivals in ((c + step2, to_second), (c + step1 + step2, to_corner)):
        for copy, (plane, rows, _) in zip(arrivals, pieces):
            pass_on(copy, plane, column, rows)
    wait_all(local + shared)

    def out_grad(j, carry):
        d = full[:, :, part(j, TILE)]
        gwo_ref[:, part(j, TILE)] = nn(o_ref[...], d.reshape(o_ref.shape[1], TILE)).astype(gwo_ref.dtype)
        return carry

    lax.fori_loop(0, tiles, out_grad, 0)

    def finish(j, carry):
        direct(j).wait()
        onward(j).wait()
        tile = part(j, TILE)
        total = (dx[z, :, tile] + above[:, tile]) + below[:, tile]
        gx_ref[:, tile] = (total + dy_ref[:, tile].astype(jnp.float32)).astype(gx_ref.dtype)
        return carry

    lax.fori_loop(0, tiles, finish, 0)


def final(dqk, dv, wqk, wv, d_ring, d_below, d_top, d_low, d_far, dqk_rows, dv_rows, o_rows, dy, x_full, collective_id):
    rows, model_dim = d_far.shape
    seq_len = x_full.shape[0]
    bf16, f32 = d_far.dtype, jnp.float32
    block = pltpu.VMEM((rows, model_dim), f32)
    scratch = [pltpu.VMEM((dqk.shape[0] // rows, rows, model_dim), f32), block, block, block,
               pltpu.VMEM((seq_len // rows, rows, model_dim), bf16), pltpu.VMEM((2, seq_len, TILE), bf16), pltpu.SemaphoreType.DMA((2, 2)),
               pltpu.SemaphoreType.DMA((SEMAPHORES,)), pltpu.SemaphoreType.DMA((SEMAPHORES,))]
    outs = (shape(dy.shape, bf16),) + (shape((model_dim, HEAD_SIZE), bf16),) * 3 + (shape((o_rows.shape[0], model_dim), bf16),)
    return call(final_kernel, outs, (dqk, dv, wqk, wv, d_ring, d_below, d_top, d_low, d_far, dqk_rows, dv_rows, o_rows, dy, x_full),
                [VMEM] * 2 + [ANY] * 7 + [VMEM] * 4 + [ANY], (VMEM,) * 5,
                scratch, collective_id, 60)


def gather_kernel(x_ref, wq_ref, wk_ref, wv_ref, wo_ref, out_ref, q_ref, k_ref, v_ref, col_ref, wqk_rows, wv_rows,
                  full, weights, rows_scr, qk_scr, total, *sems):
    me, copies = lax.axis_index('tp'), Copies(sems)
    z, c, core = position(me)
    partner = me + 1 - core * 2
    step1, step2 = ring_steps(c, core)
    first, second = me + step1 * 2, me + step2 * 2
    up, far, down = [line_peer(me, k) for k in range(1, 4)]
    planes = [z, down // 8, up // 8, far // 8]
    direct, corner = (0, 1, 3, 5), (2, 4, 6, 7)

    def slot(plane, column):
        return full.at[plane * 8 + column * 2 + core]

    own = copies.local(x_ref, slot(z, c))
    loads = [copies.local(ref, weights.at[:, pl.ds(i * HEAD_SIZE, HEAD_SIZE)]) for i, ref in enumerate((wq_ref, wk_ref, wv_ref))]
    greet([up, down, first, second, partner])
    own.wait()
    line = {i: copies.send(slot(z, c), slot(z, c), peer) for i, peer in ((1, up), (2, down))}
    to_first, to_second, to_partner, stores = {}, {}, {}, []

    def forward(s, column, index, slot_of):
        block = slot(planes[s], column)
        if index is not None:
            to_second[index] = copies.send(block, block, second)
        to_partner[slot_of] = copies.send(block, block, partner)

    def pass_on(s):
        block = slot(planes[s], c)
        to_first[s] = copies.send(block, block, first)
        forward(s, c, direct[s], s)

    def from_line(s):
        line[s].wait()
        pass_on(s)

    head, head_line, head_partner = (lambda plane: col_ref.at[plane * 2 + core]), {}, []

    def head_from_line(s):
        head_line[s].wait()
        block = head(planes[s])
        if s == 1:
            head_line[3] = copies.send(block, block, up)
        head_partner.append(copies.send(block, block, partner))

    def from_first(s):
        to_first[s].wait()
        forward(s, c + step1, corner[s], 4 + s)

    def from_second(i):
        to_second[i].wait()
        if i in direct:
            forward(direct.index(i), c + step2, None, 8 + i)
        else:
            forward(corner.index(i), c + step2 + step1, None, 8 + i)

    def multiply(s, column, slot_of):
        to_partner[slot_of].wait()
        pair = planes[s] * 4 + column
        blocks = pl.ds(pair * 2, 2)
        stores.append(copies.local(full.at[blocks], out_ref.at[blocks]))
        rows = part(pair, total.shape[0])
        total[...] = jnp.zeros_like(total)

        def chunk(i, carry):
            depth = part(i, DEPTH)
            a = full[blocks, :, depth].reshape(rows.size, DEPTH)
            total[...] += nn(a, weights[depth, :])
            return carry

        lax.fori_loop(0, weights.shape[0] // DEPTH, chunk, 0)
        qk_scr[rows, :] = total[:, :2 * HEAD_SIZE]
        v_ref[rows, :] = total[:, 2 * HEAD_SIZE:].astype(v_ref.dtype)

    def multiply_own(s):
        multiply(s, c, s)

    def multiply_sides(s):
        multiply(s, c + step1, 8 + direct[s])
        multiply(s, c + step2, 4 + s)

    def multiply_corner(s):
        multiply(s, c + step1 + step2, 8 + corner[s])

    pass_on(0)
    from_line(1)
    line[3] = copies.send(slot(planes[1], c), slot(planes[1], c), up)
    own_head = copies.local(wo_ref, head(z))
    head_line[1] = copies.send(wo_ref, head(z), up)
    head_line[2] = copies.send(wo_ref, head(z), down)
    head_partner.append(copies.send(wo_ref, head(z), partner))
    from_first(0)
    wait_all(loads)
    multiply_own(0)

    def transpose(i, carry):
        rows_scr[:, part(i, TILE)] = weights[part(i, TILE), :].T
        return carry

    lax.fori_loop(0, weights.shape[0] // TILE, transpose, 0)
    from_second(0)
    from_line(2)
    from_first(1)
    multiply_own(1)
    from_second(1)
    from_first(2)
    from_line(3)
    stores.append(copies.local(rows_scr.at[pl.ds(0, 2 * HEAD_SIZE), :], wqk_rows))
    stores.append(copies.local(rows_scr.at[pl.ds(2 * HEAD_SIZE, HEAD_SIZE), :], wv_rows))
    multiply_own(2)
    from_second(2)
    head_from_line(1)
    multiply_sides(0)
    from_first(3)
    multiply_own(3)
    from_second(3)
    multiply_sides(1)
    from_second(4)
    multiply_corner(0)
    from_second(5)
    multiply_sides(2)
    head_from_line(2)
    from_second(6)
    multiply_sides(3)
    multiply_corner(1)
    from_second(7)
    multiply_corner(2)
    multiply_corner(3)

    def turn(i, carry):
        values = qk_scr[part(i, TILE), :].T
        q_ref[:, part(i, TILE)] = values[:HEAD_SIZE]
        k_ref[:, part(i, TILE)] = values[HEAD_SIZE:]
        return carry

    lax.fori_loop(0, qk_scr.shape[0] // TILE, turn, 0)
    head_from_line(3)
    wait_all(stores + [own_head] + head_partner)


def gather(x, wq, wk, wv, wo, devices, collective_id):
    rows, model_dim = x.shape
    f32 = jnp.float32
    head = (devices * rows, HEAD_SIZE)
    outs = (shape((devices, rows, model_dim), x.dtype), shape(head[::-1], f32), shape(head[::-1], f32), shape(head, x.dtype),
            shape((8,) + wo.shape, wo.dtype), shape((2 * HEAD_SIZE, model_dim), x.dtype), shape((HEAD_SIZE, model_dim), x.dtype))
    width = 3 * HEAD_SIZE
    scratch = [pltpu.VMEM((devices, rows, model_dim), x.dtype), pltpu.VMEM((model_dim, width), x.dtype),
               pltpu.VMEM((width, model_dim), x.dtype), pltpu.VMEM((devices * rows, 2 * HEAD_SIZE), f32), pltpu.VMEM((2 * rows, width), f32)]
    return call(gather_kernel, outs, (x, wq, wk, wv, wo), [ANY] * 5, (ANY, VMEM, VMEM, VMEM, ANY, ANY, ANY), scratch, collective_id, 62)


def nt(a, b):
    return lax.dot_general(a, b, (((1,), (1,)), ((), ())), preferred_element_type=jnp.float32)


def tn(a, b):
    return lax.dot_general(a, b, (((0,), (0,)), ((), ())), preferred_element_type=jnp.float32)


def nn(a, b):
    return lax.dot_general(a, b, (((1,), (0,)), ((), ())), preferred_element_type=jnp.float32)


def fold_rows(values, op):
    return op(values.reshape(values.shape[0] // 8, 8, values.shape[1]), axis=0)


def block_rows(j):
    return pl.ds(pl.multiple_of(j * BLOCK, BLOCK), BLOCK)


def diagonal_mask():
    keys = lax.broadcasted_iota(jnp.int32, (BLOCK, BLOCK), 0)
    queries = lax.broadcasted_iota(jnp.int32, (BLOCK, BLOCK), 1)
    return keys <= queries


def attention_kernel(q_ref, k_ref, v_ref, o_ref, ot_ref, max_ref, inv_ref, s_scr, acc_scr):
    i = pl.program_id(0)
    q_blk = q_ref[...]

    def score(j, top):
        s = tn(k_ref[:, block_rows(j)], q_blk) * (ATTN_SCALE * LOG2E)
        s_scr[block_rows(j), :] = s
        return jnp.maximum(top, fold_rows(s, jnp.max))

    s = jnp.where(diagonal_mask(), tn(k_ref[:, block_rows(i)], q_blk) * (ATTN_SCALE * LOG2E), -1e30)
    s_scr[block_rows(i), :] = s
    top = lax.fori_loop(0, i, score, fold_rows(s, jnp.max))
    top = jnp.max(top, axis=0, keepdims=True)

    def weigh(j, total):
        p = jnp.exp2(s_scr[block_rows(j), :] - top)
        s_scr[block_rows(j), :] = p
        return total + fold_rows(p, jnp.sum)

    total = lax.fori_loop(0, i + 1, weigh, jnp.zeros((8, BLOCK), jnp.float32))
    inv = 1.0 / jnp.sum(total, axis=0, keepdims=True)
    max_ref[...] = top
    inv_ref[...] = inv
    acc_scr[...] = jnp.zeros_like(acc_scr)

    def gather(j, carry):
        p = (s_scr[block_rows(j), :] * inv).astype(jnp.bfloat16)
        acc_scr[...] += tn(v_ref[block_rows(j), :], p)
        return carry

    lax.fori_loop(0, i + 1, gather, 0)
    o_ref[...] = acc_scr[...].T.astype(jnp.bfloat16)
    ot_ref[...] = acc_scr[...].astype(jnp.bfloat16)


def attention(q, k, v):
    seq_len = v.shape[0]
    steps = seq_len // BLOCK
    rows = pl.BlockSpec((BLOCK, HEAD_SIZE), lambda i: (i, 0))
    whole = pl.BlockSpec((seq_len, HEAD_SIZE), lambda i: (0, 0))
    line = pl.BlockSpec((1, BLOCK), lambda i: (0, i))
    columns = pl.BlockSpec((HEAD_SIZE, BLOCK), lambda i: (0, i))
    wide = pl.BlockSpec((HEAD_SIZE, seq_len), lambda i: (0, 0))
    return pl.pallas_call(
        attention_kernel,
        grid=(steps,),
        out_shape=(jax.ShapeDtypeStruct((seq_len, HEAD_SIZE), jnp.bfloat16),
                   jax.ShapeDtypeStruct((HEAD_SIZE, seq_len), jnp.bfloat16),
                   jax.ShapeDtypeStruct((1, seq_len), jnp.float32),
                   jax.ShapeDtypeStruct((1, seq_len), jnp.float32)),
        in_specs=[columns, wide, whole], out_specs=(rows, columns, line, line),
        scratch_shapes=[pltpu.VMEM((seq_len, BLOCK), jnp.float32), pltpu.VMEM((HEAD_SIZE, BLOCK), jnp.float32)],
        compiler_params=pltpu.CompilerParams(dimension_semantics=("arbitrary",), vmem_limit_bytes=40 << 20),
        cost_estimate=pl.CostEstimate(flops=8 * seq_len * seq_len * HEAD_SIZE, bytes_accessed=8 * seq_len * HEAD_SIZE, transcendentals=0),
    )(q, k, v)


def attention_grad_kernel(q_ref, k_ref, v_ref, do_ref, max_ref, inv_ref, dq_ref, dk_ref, dv_ref, dvt_ref, p_scr, dp_scr, dq_scr, dk_scr, dv_scr):
    i = pl.program_id(0)
    q_blk, do_blk = q_ref[...], do_ref[...]
    top, inv = max_ref[...], inv_ref[...]

    @pl.when(i == 0)
    def _():
        dk_scr[...] = jnp.zeros_like(dk_scr)
        dv_scr[...] = jnp.zeros_like(dv_scr)

    def scores(j, mask, delta):
        rows = block_rows(j)
        s = tn(k_ref[:, rows], q_blk) * (ATTN_SCALE * LOG2E)
        if mask is not None:
            s = jnp.where(mask, s, -1e30)
        p = jnp.exp2(s - top) * inv
        dp = nt(v_ref[rows, :], do_blk)
        p_scr[rows, :] = p
        dp_scr[rows, :] = dp
        dv_scr[rows, :] += nn(p.astype(jnp.bfloat16), do_blk)
        return delta + fold_rows(p * dp, jnp.sum)

    delta = scores(i, diagonal_mask(), jnp.zeros((8, BLOCK), jnp.float32))
    delta = lax.fori_loop(0, i, lambda j, d: scores(j, None, d), delta)
    delta = jnp.sum(delta, axis=0, keepdims=True)
    dq_scr[...] = jnp.zeros_like(dq_scr)

    def grads(j, carry):
        rows = block_rows(j)
        ds = (p_scr[rows, :] * (dp_scr[rows, :] - delta) * ATTN_SCALE).astype(jnp.bfloat16)
        dk_scr[:, rows] += nt(q_blk, ds)
        dq_scr[...] += nn(k_ref[:, rows], ds)
        return carry

    lax.fori_loop(0, i + 1, grads, 0)
    dq_ref[...] = dq_scr[...]

    @pl.when(i == pl.num_programs(0) - 1)
    def _():
        dk_ref[...] = dk_scr[...]
        dv_ref[...] = dv_scr[...].astype(jnp.bfloat16)

        def turn(j, carry):
            dvt_ref[:, block_rows(j)] = dv_scr[block_rows(j), :].T.astype(jnp.bfloat16)
            return carry

        lax.fori_loop(0, pl.num_programs(0), turn, 0)


def attention_grad(q, k, v, do, top, inv):
    seq_len = v.shape[0]
    steps = seq_len // BLOCK
    rows = pl.BlockSpec((BLOCK, HEAD_SIZE), lambda i: (i, 0))
    whole = pl.BlockSpec((seq_len, HEAD_SIZE), lambda i: (0, 0))
    line = pl.BlockSpec((1, BLOCK), lambda i: (0, i))
    columns = pl.BlockSpec((HEAD_SIZE, BLOCK), lambda i: (0, i))
    wide = pl.BlockSpec((HEAD_SIZE, seq_len), lambda i: (0, 0))
    full, turned = (seq_len, HEAD_SIZE), (HEAD_SIZE, seq_len)
    return pl.pallas_call(
        attention_grad_kernel,
        grid=(steps,),
        out_shape=(shape(turned, jnp.float32), shape(turned, jnp.float32), shape(full, jnp.bfloat16), shape(turned, jnp.bfloat16)),
        in_specs=[columns, wide, whole, rows, line, line], out_specs=(columns, wide, whole, wide),
        scratch_shapes=[pltpu.VMEM((seq_len, BLOCK), jnp.float32), pltpu.VMEM((seq_len, BLOCK), jnp.float32),
                        pltpu.VMEM((HEAD_SIZE, BLOCK), jnp.float32), pltpu.VMEM(turned, jnp.float32), pltpu.VMEM(full, jnp.float32)],
        compiler_params=pltpu.CompilerParams(dimension_semantics=("arbitrary",), vmem_limit_bytes=48 << 20),
        cost_estimate=pl.CostEstimate(flops=20 * seq_len * seq_len * HEAD_SIZE, bytes_accessed=20 * seq_len * HEAD_SIZE, transcendentals=0),
    )(q, k, v, do, top, inv)


COLUMN_GROUPS = [[z * 8 + c * 2 + core for z in range(4) for core in range(2)] for c in range(4)]
PLANE_GROUPS = [[z * 8 + p for p in range(8)] for z in range(4)]


def lane_rows(values):
    return values.reshape(-1, 128)


def local_block(x_loc, wq_loc, wk_loc, wv_loc, wo_loc, gq_loc, gk_loc, g_attn, dy_loc):
    x_loc, dy_loc = x_loc[0], dy_loc[0]
    rows, model_dim = x_loc.shape
    bf16, f32 = jnp.bfloat16, jnp.float32
    x_blocks, q_raw, k_raw, v_head, wo_blocks, wqk_rows, wv_rows = gather(x_loc, wq_loc, wk_loc, wv_loc, wo_loc, 32, 9)
    wo_col = wo_blocks.reshape(8 * HEAD_SIZE, model_dim)
    x_full = x_blocks.reshape(32 * rows, model_dim)
    seq_len = x_full.shape[0]
    wv_plane = lax.all_gather(wv_rows, 'tp', axis=0, tiled=True, axis_index_groups=PLANE_GROUPS)
    cos_t, sin_t = rope_tables(seq_len)
    stats = jnp.concatenate([lane_rows(jnp.sum(q_raw * q_raw, axis=0)), lane_rows(jnp.sum(k_raw * k_raw, axis=0))])
    sq_sums = all_sum(stats, 1).reshape(2, seq_len)
    inv_rms = lax.rsqrt(sq_sums / model_dim + NORM_EPS)[:, None, :]
    q_unit = q_raw * inv_rms[0]
    k_unit = k_raw * inv_rms[1]
    gq_f, gk_f = gq_loc.astype(f32)[:, None], gk_loc.astype(f32)[:, None]
    q_rot = rotate(q_unit * gq_f, cos_t, sin_t).astype(bf16)
    k_rot = rotate(k_unit * gk_f, cos_t, sin_t).astype(bf16)
    o_head, o_rows, top, inv = attention(q_rot, k_rot, v_head)

    o_col = exchange(
        o_head.reshape(4, 4, 2, rows, HEAD_SIZE), (4, rows, 8 * HEAD_SIZE), column_peer, 8,
        lambda ref, d: ref.at[d // 8, :, d % 2],
        lambda ref, d: ref.at[:, :, part(member_of(d), HEAD_SIZE)], 2)
    a_part = nn(o_col.reshape(4 * rows, 8 * HEAD_SIZE), wo_col)
    attn_loc = ring_sum(a_part.reshape(4, rows, model_dim), 3)

    post_rms = lax.rsqrt(jnp.mean(attn_loc * attn_loc, axis=-1, keepdims=True) + NORM_EPS)
    normed = attn_loc * post_rms
    ga_f = g_attn.astype(f32)
    dy_f = dy_loc.astype(f32)
    y_loc = (x_loc.astype(f32) + normed * ga_f).astype(bf16)
    ga_part = jnp.sum(dy_f * normed, axis=0)
    g_normed = dy_f * ga_f
    d_attn = (post_rms * (g_normed - normed * jnp.mean(g_normed * normed, axis=-1, keepdims=True))).astype(bf16)

    d_ring, d_below, d_top, wqk_after = spread(d_attn, wqk_rows, 4)
    wqk_plane = lax.all_gather(wqk_after, 'tp', axis=0, tiled=True, axis_index_groups=PLANE_GROUPS)
    d_col = nt(d_ring.reshape(4 * rows, model_dim), wo_col).astype(bf16)
    d_head = exchange(
        d_col.reshape(4, rows, 8 * HEAD_SIZE), (4, 4, 2, rows, HEAD_SIZE), column_peer, 8,
        lambda ref, d: ref.at[:, :, part(member_of(d), HEAD_SIZE)],
        lambda ref, d: ref.at[d // 8, :, d % 2], 5).reshape(seq_len, HEAD_SIZE)

    dq_rot, dk_rot, d_value, d_value_rows = attention_grad(q_rot, k_rot, v_head, d_head, top, inv)
    dq_hat = rotate_back(dq_rot, cos_t, sin_t)
    dk_hat = rotate_back(dk_rot, cos_t, sin_t)
    grad_gq = jnp.sum(dq_hat * q_unit, axis=1)
    grad_gk = jnp.sum(dk_hat * k_unit, axis=1)
    dq_unit = dq_hat * gq_f
    dk_unit = dk_hat * gk_f
    sums = jnp.concatenate([lane_rows(jnp.sum(dq_unit * q_unit, axis=0)), lane_rows(jnp.sum(dk_unit * k_unit, axis=0)), lane_rows(ga_part)])
    sums = all_sum(sums, 6)
    dots_rows = 2 * seq_len // 128
    unit_dots = sums[:dots_rows].reshape(2, seq_len)[:, None, :] / model_dim
    grad_ga = sums[dots_rows:].reshape(model_dim)
    dq_raw = (inv_rms[0] * (dq_unit - q_unit * unit_dots[0])).astype(bf16)
    dk_raw = (inv_rms[1] * (dk_unit - k_unit * unit_dots[1])).astype(bf16)
    dqk_rows = jnp.concatenate([dq_raw, dk_raw], axis=0)
    d_qk = dqk_rows.T

    dqk_plane, dv_plane, d_far, d_low = plane_exchange(
        d_qk.reshape(4, 8, rows, 2 * HEAD_SIZE), d_value.reshape(4, 8, rows, HEAD_SIZE), d_below, d_attn, 7)
    grad_x, grad_wq, grad_wk, grad_wv, grad_wo = final(
        dqk_plane.reshape(4 * rows, 16 * HEAD_SIZE), dv_plane.reshape(4 * rows, 8 * HEAD_SIZE), wqk_plane, wv_plane,
        d_ring, d_below, d_top, d_low, d_far, dqk_rows, d_value_rows, o_rows, dy_loc, x_full, 8)
    return (y_loc[None], grad_x[None], grad_wq, grad_wk, grad_wv, grad_wo,
            grad_gq.astype(bf16), grad_gk.astype(bf16), grad_ga.astype(bf16))


def solution(mesh):
    act_spec = P(None, 'tp', None)
    col_spec = P(None, 'tp')
    row_spec = P('tp', None)
    vec_spec = P('tp')
    in_specs = (act_spec, col_spec, col_spec, col_spec, row_spec, vec_spec, vec_spec, P(), act_spec)
    out_specs = (act_spec, act_spec, col_spec, col_spec, col_spec, row_spec, vec_spec, vec_spec, P())
    return jax.shard_map(local_block, mesh=mesh, in_specs=in_specs, out_specs=out_specs, check_vma=False)
```

```python
import functools

import jax
import jax.numpy as jnp
from jax import lax
from jax.experimental import pallas as pl
from jax.experimental.pallas import tpu as pltpu
from jax.sharding import PartitionSpec as P

HEAD_SIZE = 128
ROPE_THETA = 500000.0
NORM_EPS = 1e-6
LOG2E = 1.4426950408889634
ATTN_SCALE = HEAD_SIZE ** -0.5
MESH = pl.DeviceIdType.MESH
VMEM = pl.BlockSpec(memory_space=pltpu.VMEM)
BLOCK = 512


def rope_tables(seq_len):
    half_dim = HEAD_SIZE // 2
    inv_freq = 1.0 / (ROPE_THETA ** (jnp.arange(half_dim, dtype=jnp.float32) / half_dim))
    angles = inv_freq[:, None] * jnp.arange(seq_len, dtype=jnp.float32)[None, :]
    return jnp.cos(angles), jnp.sin(angles)


def rotate(values, cos_t, sin_t):
    lower_half, upper_half = jnp.split(values, 2, axis=0)
    return jnp.concatenate([lower_half * cos_t - upper_half * sin_t, upper_half * cos_t + lower_half * sin_t], axis=0)


def rotate_back(values, cos_t, sin_t):
    return rotate(values, cos_t, -sin_t)


SEMAPHORES = 72
DEPTH = 1024
CHUNKS = 4
TILE = 512
ANY = pl.BlockSpec(memory_space=pl.ANY)


def position(d):
    return d // 8, d // 2 % 4, d % 2


def member_of(d):
    z, _, core = position(d)
    return z * 2 + core


def column_peer(me, k):
    member = (member_of(me) + k) % 8
    return member // 2 * 8 + position(me)[1] * 2 + member % 2


def plane_peer(me, k):
    return me - me % 8 + (me + k) % 8


def line_peer(me, k):
    return (me + k * 8) % 32


def ring_steps(c, core):
    step_x, step_y = 1 - c % 2 * 2, 2 - c // 2 * 4
    step1 = step_x * (1 - core) + step_y * core
    return step1, step_x + step_y - step1


def greet(peers):
    barrier = pltpu.get_barrier_semaphore()
    for peer in peers:
        pl.semaphore_signal(barrier, inc=1, device_id=(peer,), device_id_type=MESH)
    pl.semaphore_wait(barrier, len(peers))


def remote(src, dst, sems, slot, peer):
    return pltpu.make_async_remote_copy(
        src_ref=src, dst_ref=dst, send_sem=sems[0].at[slot], recv_sem=sems[1].at[slot], device_id=(peer,), device_id_type=MESH)


class Copies:
    def __init__(self, sems):
        self.sems, self.used = sems, 0

    def send(self, src, dst, peer):
        copy = remote(src, dst, self.sems, self.used, peer)
        copy.start()
        self.used += 1
        return copy

    def local(self, src, dst):
        copy = pltpu.make_async_copy(src, dst, self.sems[2].at[self.used])
        copy.start()
        self.used += 1
        return copy


def wait_all(copies):
    for copy in copies:
        copy.wait()


def call(kernel, out_shape, operands, in_specs, out_specs, scratch, collective_id, mib):
    return pl.pallas_call(
        kernel, out_shape=out_shape, in_specs=in_specs, out_specs=out_specs,
        scratch_shapes=list(scratch) + [pltpu.SemaphoreType.DMA((SEMAPHORES,))] * 3,
        compiler_params=pltpu.CompilerParams(collective_id=collective_id, has_side_effects=True, vmem_limit_bytes=mib << 20),
    )(*operands)


def shape(dims, dtype):
    return jax.ShapeDtypeStruct(tuple(dims), dtype)


def part(index, size):
    return pl.ds(pl.multiple_of(index * size, size), size)


def add_rows(ref, other, start, count):
    def add(i, carry):
        rows = part(start // 8 + i, 8)
        ref[rows, :] = ref[rows, :] + other[rows, :]
        return carry

    lax.fori_loop(0, count // 8, add, 0)


def exchange_kernel(peer_of, count, source, target, x_ref, out_ref, *sems):
    me, copies = lax.axis_index('tp'), Copies(sems)
    peers = [peer_of(me, k) for k in range(1, count)]
    greet(peers)
    started = [copies.send(source(x_ref, peer), target(out_ref, me), peer) for peer in peers]
    target(out_ref, me)[...] = source(x_ref, me)[...]
    wait_all(started)


def exchange(x, out_shape, peer_of, count, source, target, collective_id):
    kernel = functools.partial(exchange_kernel, peer_of, count, source, target)
    return call(kernel, shape(out_shape, x.dtype), (x,), [VMEM], VMEM, [], collective_id, 24)


def all_sum_kernel(x_ref, out_ref, plane, middle, line, *sems):
    me, copies = lax.axis_index('tp'), Copies(sems)
    z, mine = me // 8, me % 8
    plane_peers = [plane_peer(me, k) for k in range(1, 8)]
    line_peers = [line_peer(me, k) for k in range(1, 4)]
    greet(plane_peers + line_peers)
    started = [copies.send(x_ref, plane.at[mine], peer) for peer in plane_peers]
    plane[mine] = x_ref[...]
    wait_all(started)
    total = plane[0]
    for k in range(1, 8):
        total = total + plane[k]
    middle[...] = total
    line[z] = total
    wait_all([copies.send(middle, line.at[z], peer) for peer in line_peers])
    out_ref[...] = (line[0] + line[1]) + (line[2] + line[3])


def all_sum(x, collective_id):
    scratch = [pltpu.VMEM((8,) + x.shape, x.dtype), pltpu.VMEM(x.shape, x.dtype), pltpu.VMEM((4,) + x.shape, x.dtype)]
    return call(all_sum_kernel, shape(x.shape, x.dtype), (x,), [VMEM], VMEM, scratch, collective_id, 8)


def ring_sum_kernel(x_ref, out_ref, passing, direct, last, *sems):
    me, copies = lax.axis_index('tp'), Copies(sems)
    _, c, core = position(me)
    step1, step2 = ring_steps(c, core)
    first, second = me + step1 * 2, me + step2 * 2
    greet([first, second])
    chunk = out_ref.shape[0] // CHUNKS
    pieces = [pl.ds(i * chunk, chunk) for i in range(CHUNKS)]
    hops = [copies.send(x_ref.at[c + step1 + step2, p, :], passing.at[p, :], first) for p in pieces]
    sums = [copies.send(x_ref.at[c + step1], direct, first)]
    for i, p in enumerate(pieces):
        hops[i].wait()
        add_rows(passing, x_ref.at[c + step2], i * chunk, chunk)
        sums.append(copies.send(passing.at[p, :], last.at[p, :], second))
    wait_all(sums)

    def add(i, carry):
        rows = part(i, 8)
        out_ref[rows, :] = (x_ref[c, rows, :] + direct[rows, :]) + last[rows, :]
        return carry

    lax.fori_loop(0, out_ref.shape[0] // 8, add, 0)


def ring_sum(x, collective_id):
    dims = x.shape[1:]
    return call(ring_sum_kernel, shape(dims, x.dtype), (x,), [VMEM], VMEM, [pltpu.VMEM(dims, x.dtype)] * 3, collective_id, 32)


def spread_kernel(x_ref, w_ref, ring_ref, below_ref, above_ref, w_out, *sems):
    me, copies = lax.axis_index('tp'), Copies(sems)
    _, c, core = position(me)
    step1, step2 = ring_steps(c, core)
    first, second = me + step1 * 2, me + step2 * 2
    up, down = line_peer(me, 1), line_peer(me, 3)
    greet([first, second, up, down])
    forth = copies.send(x_ref, ring_ref.at[c], first)
    started = [copies.send(x_ref, ring_ref.at[c], second), copies.send(x_ref, below_ref, up),
               copies.send(x_ref.at[pl.ds(0, above_ref.shape[0]), :], above_ref, down)]
    held = copies.local(w_ref, w_out)
    ring_ref[c] = x_ref[...]
    forth.wait()
    block = ring_ref.at[c + step1]
    wait_all(started + [copies.send(block, block, second), held])


def spread(x, w, collective_id):
    half = shape((x.shape[0] // 2, x.shape[1]), x.dtype)
    outs = (shape((4,) + x.shape, x.dtype), shape(x.shape, x.dtype), half, shape(w.shape, w.dtype))
    return call(spread_kernel, outs, (x, w), [VMEM, ANY], (VMEM, ANY, ANY, ANY), [], collective_id, 24)


def plane_kernel(qk_ref, v_ref, below_ref, d_ref, out_qk, out_v, far_ref, above_ref, *sems):
    me, copies = lax.axis_index('tp'), Copies(sems)
    peers = [plane_peer(me, k) for k in range(1, 8)]
    up, down = line_peer(me, 1), line_peer(me, 3)
    greet(peers + [up, down])
    mine = me % 8
    started = [copies.send(below_ref, far_ref, up), copies.send(d_ref.at[pl.ds(above_ref.shape[0], above_ref.shape[0]), :], above_ref, down)]
    for src, dst in ((qk_ref, out_qk), (v_ref, out_v)):
        columns = part(mine, src.shape[-1])
        started += [copies.send(src.at[:, peer % 8], dst.at[:, :, columns], peer) for peer in peers]
        started.append(copies.local(src.at[:, mine], dst.at[:, :, columns]))
    wait_all(started)


def plane_exchange(qk, v, below, d, collective_id):
    outs = tuple(shape((4, a.shape[2], 8 * a.shape[3]), a.dtype) for a in (qk, v)) + (
        shape(below.shape, below.dtype), shape((d.shape[0] // 2, d.shape[1]), d.dtype))
    return call(plane_kernel, outs, (qk, v, below, d), [VMEM, VMEM, ANY, ANY], (ANY,) * 4, [], collective_id, 62)


def final_kernel(dqk_ref, dv_ref, wqk_ref, wv_ref, ring_ref, below_ref, top_ref, low_ref, far_ref, dwqk_ref, dwv_ref, o_ref, dy_ref, x_ref,
                 gx_ref, gwq_ref, gwk_ref, gwv_ref, gwo_ref,
                 dx, above, below, passing, full, buf, tile_sem, line_send, line_recv, *sems):
    me, copies = lax.axis_index('tp'), Copies(sems)
    z, c, core = position(me)
    partner = me + 1 - core * 2
    up, down = line_peer(me, 1), line_peer(me, 3)
    z_up, z_far, z_down = up // 8, line_peer(me, 2) // 8, down // 8
    step1, step2 = ring_steps(c, core)
    first, second = me + step1 * 2, me + step2 * 2
    greet([up, down, partner, first, second])
    tiles = x_ref.shape[1] // TILE
    depth = dqk_ref.shape[1]
    line_sems = (line_send, line_recv)

    def fetch_w(j, b):
        return [pltpu.make_async_copy(wqk_ref.at[:, part(j, TILE)], buf.at[b, pl.ds(0, depth), :], tile_sem.at[0, b]),
                pltpu.make_async_copy(wv_ref.at[:, part(j, TILE)], buf.at[b, pl.ds(depth, dv_ref.shape[1]), :], tile_sem.at[1, b])]

    def fetch_x(j, b):
        return [pltpu.make_async_copy(x_ref.at[:, part(j, TILE)], buf.at[b], tile_sem.at[0, b])]

    for copy in fetch_w(0, 0):
        copy.start()
    half = top_ref.shape[0]
    whole = pl.ds(0, 2 * half)
    pieces = [(z_down, whole, below_ref), (z_up, pl.ds(0, half), top_ref), (z_up, pl.ds(half, half), low_ref), (z_far, whole, far_ref)]

    def spot(plane, column, rows):
        return full.at[plane * 8 + column * 2 + core, rows, :]

    to_first = [copies.send(block, spot(plane, c, rows), first) for plane, rows, block in pieces]
    to_second = [copies.send(block, spot(plane, c, rows), second) for plane, rows, block in pieces]
    to_corner, shared, local = [], [], []
    held = [(block, spot(plane, c, rows)) for plane, rows, block in pieces]
    held += [(ring_ref.at[column], spot(z, column, whole)) for column in range(4)]
    for block, place in held:
        shared.append(copies.send(block, place, partner))
        local.append(copies.local(block, place))

    def pass_on(copy, plane, column, rows):
        copy.wait()
        block = spot(plane, column, rows)
        shared.append(copies.send(block, block, partner))
        return block

    def hop(j):
        return remote(dx.at[z_far, :, part(j, TILE)], passing.at[:, part(j, TILE)], line_sems, j, up)

    def direct(j):
        return remote(dx.at[z_down, :, part(j, TILE)], above.at[:, part(j, TILE)], line_sems, tiles + j, down)

    def onward(j):
        return remote(passing.at[:, part(j, TILE)], below.at[:, part(j, TILE)], line_sems, tiles * 2 + j, up)

    def input_grad(j, carry):
        b = j % 2

        @pl.when(j + 1 < tiles)
        def _():
            for copy in fetch_w(j + 1, 1 - b):
                copy.start()

        wait_all(fetch_w(j, b))
        values = nn(dqk_ref[...], buf[b, :depth, :]) + nn(dv_ref[...], buf[b, depth:, :])
        dx[:, :, part(j, TILE)] = values.reshape(dx.shape[0], dx.shape[1], TILE)

        @pl.when(j > 0)
        def _():
            hop(j - 1).start()
            direct(j - 1).start()

        return carry

    lax.fori_loop(0, tiles, input_grad, 0)
    for copy in fetch_x(0, 0):
        copy.start()

    def weight_grad(j, carry):
        b = j % 2

        @pl.when(j + 1 < tiles)
        def _():
            for copy in fetch_x(j + 1, 1 - b):
                copy.start()

        wait_all(fetch_x(j, b))

        @pl.when(j == 0)
        def _():
            hop(tiles - 1).start()
            direct(tiles - 1).start()

        hop(j).wait()
        passing[:, part(j, TILE)] = passing[:, part(j, TILE)] + dx[z_up, :, part(j, TILE)]
        values = nn(dwqk_ref[...], buf[b]).T
        gwq_ref[part(j, TILE), :] = values[:, :HEAD_SIZE].astype(gwq_ref.dtype)
        gwk_ref[part(j, TILE), :] = values[:, HEAD_SIZE:].astype(gwk_ref.dtype)
        gwv_ref[part(j, TILE), :] = nn(dwv_ref[...], buf[b]).T.astype(gwv_ref.dtype)
        onward(j).start()
        return carry

    lax.fori_loop(0, tiles, weight_grad, 0)
    for copy, (plane, rows, _) in zip(to_first, pieces):
        block = pass_on(copy, plane, c + step1, rows)
        to_corner.append(copies.send(block, block, second))
    for column, arrivals in ((c + step2, to_second), (c + step1 + step2, to_corner)):
        for copy, (plane, rows, _) in zip(arrivals, pieces):
            pass_on(copy, plane, column, rows)
    wait_all(local + shared)

    def out_grad(j, carry):
        d = full[:, :, part(j, TILE)]
        gwo_ref[:, part(j, TILE)] = nn(o_ref[...], d.reshape(o_ref.shape[1], TILE)).astype(gwo_ref.dtype)
        return carry

    lax.fori_loop(0, tiles, out_grad, 0)

    def finish(j, carry):
        direct(j).wait()
        onward(j).wait()
        tile = part(j, TILE)
        total = (dx[z, :, tile] + above[:, tile]) + below[:, tile]
        gx_ref[:, tile] = (total + dy_ref[:, tile].astype(jnp.float32)).astype(gx_ref.dtype)
        return carry

    lax.fori_loop(0, tiles, finish, 0)


def final(dqk, dv, wqk, wv, d_ring, d_below, d_top, d_low, d_far, dqk_rows, dv_rows, o_rows, dy, x_full, collective_id):
    rows, model_dim = d_far.shape
    seq_len = x_full.shape[0]
    bf16, f32 = d_far.dtype, jnp.float32
    block = pltpu.VMEM((rows, model_dim), f32)
    scratch = [pltpu.VMEM((dqk.shape[0] // rows, rows, model_dim), f32), block, block, block,
               pltpu.VMEM((seq_len // rows, rows, model_dim), bf16), pltpu.VMEM((2, seq_len, TILE), bf16), pltpu.SemaphoreType.DMA((2, 2)),
               pltpu.SemaphoreType.DMA((SEMAPHORES,)), pltpu.SemaphoreType.DMA((SEMAPHORES,))]
    outs = (shape(dy.shape, bf16),) + (shape((model_dim, HEAD_SIZE), bf16),) * 3 + (shape((o_rows.shape[0], model_dim), bf16),)
    return call(final_kernel, outs, (dqk, dv, wqk, wv, d_ring, d_below, d_top, d_low, d_far, dqk_rows, dv_rows, o_rows, dy, x_full),
                [VMEM] * 2 + [ANY] * 7 + [VMEM] * 4 + [ANY], (VMEM,) * 5,
                scratch, collective_id, 60)


def gather_kernel(x_ref, wq_ref, wk_ref, wv_ref, wo_ref, out_ref, q_ref, k_ref, v_ref, col_ref, wqk_rows, wv_rows,
                  full, weights, rows_scr, qk_scr, total, *sems):
    me, copies = lax.axis_index('tp'), Copies(sems)
    z, c, core = position(me)
    partner = me + 1 - core * 2
    step1, step2 = ring_steps(c, core)
    first, second = me + step1 * 2, me + step2 * 2
    up, far, down = [line_peer(me, k) for k in range(1, 4)]
    planes = [z, down // 8, up // 8, far // 8]
    direct, corner = (0, 1, 3, 5), (2, 4, 6, 7)

    def slot(plane, column):
        return full.at[plane * 8 + column * 2 + core]

    own = copies.local(x_ref, slot(z, c))
    loads = [copies.local(ref, weights.at[:, pl.ds(i * HEAD_SIZE, HEAD_SIZE)]) for i, ref in enumerate((wq_ref, wk_ref, wv_ref))]
    greet([up, down, first, second, partner])
    own.wait()
    line = {i: copies.send(slot(z, c), slot(z, c), peer) for i, peer in ((1, up), (2, down))}
    to_first, to_second, to_partner, stores = {}, {}, {}, []

    def forward(s, column, index, slot_of):
        block = slot(planes[s], column)
        if index is not None:
            to_second[index] = copies.send(block, block, second)
        to_partner[slot_of] = copies.send(block, block, partner)

    def pass_on(s):
        block = slot(planes[s], c)
        to_first[s] = copies.send(block, block, first)
        forward(s, c, direct[s], s)

    def from_line(s):
        line[s].wait()
        pass_on(s)

    head, head_line, head_partner = (lambda plane: col_ref.at[plane * 2 + core]), {}, []

    def head_from_line(s):
        head_line[s].wait()
        block = head(planes[s])
        if s == 1:
            head_line[3] = copies.send(block, block, up)
        head_partner.append(copies.send(block, block, partner))

    def from_first(s):
        to_first[s].wait()
        forward(s, c + step1, corner[s], 4 + s)

    def from_second(i):
        to_second[i].wait()
        if i in direct:
            forward(direct.index(i), c + step2, None, 8 + i)
        else:
            forward(corner.index(i), c + step2 + step1, None, 8 + i)

    def multiply(s, column, slot_of):
        to_partner[slot_of].wait()
        pair = planes[s] * 4 + column
        blocks = pl.ds(pair * 2, 2)
        stores.append(copies.local(full.at[blocks], out_ref.at[blocks]))
        rows = part(pair, total.shape[0])
        total[...] = jnp.zeros_like(total)

        def chunk(i, carry):
            depth = part(i, DEPTH)
            a = full[blocks, :, depth].reshape(rows.size, DEPTH)
            total[...] += nn(a, weights[depth, :])
            return carry

        lax.fori_loop(0, weights.shape[0] // DEPTH, chunk, 0)
        qk_scr[rows, :] = total[:, :2 * HEAD_SIZE]
        v_ref[rows, :] = total[:, 2 * HEAD_SIZE:].astype(v_ref.dtype)

    def multiply_own(s):
        multiply(s, c, s)

    def multiply_sides(s):
        multiply(s, c + step1, 8 + direct[s])
        multiply(s, c + step2, 4 + s)

    def multiply_corner(s):
        multiply(s, c + step1 + step2, 8 + corner[s])

    pass_on(0)
    from_line(1)
    line[3] = copies.send(slot(planes[1], c), slot(planes[1], c), up)
    own_head = copies.local(wo_ref, head(z))
    head_line[1] = copies.send(wo_ref, head(z), up)
    head_line[2] = copies.send(wo_ref, head(z), down)
    head_partner.append(copies.send(wo_ref, head(z), partner))
    from_first(0)
    wait_all(loads)
    multiply_own(0)

    def transpose(i, carry):
        rows_scr[:, part(i, TILE)] = weights[part(i, TILE), :].T
        return carry

    lax.fori_loop(0, weights.shape[0] // TILE, transpose, 0)
    from_second(0)
    from_line(2)
    from_first(1)
    multiply_own(1)
    from_second(1)
    from_first(2)
    from_line(3)
    stores.append(copies.local(rows_scr.at[pl.ds(0, 2 * HEAD_SIZE), :], wqk_rows))
    stores.append(copies.local(rows_scr.at[pl.ds(2 * HEAD_SIZE, HEAD_SIZE), :], wv_rows))
    multiply_own(2)
    from_second(2)
    head_from_line(1)
    multiply_sides(0)
    from_first(3)
    multiply_own(3)
    from_second(3)
    multiply_sides(1)
    from_second(4)
    multiply_corner(0)
    from_second(5)
    multiply_sides(2)
    head_from_line(2)
    from_second(6)
    multiply_sides(3)
    multiply_corner(1)
    from_second(7)
    multiply_corner(2)
    multiply_corner(3)

    def turn(i, carry):
        values = qk_scr[part(i, TILE), :].T
        q_ref[:, part(i, TILE)] = values[:HEAD_SIZE]
        k_ref[:, part(i, TILE)] = values[HEAD_SIZE:]
        return carry

    lax.fori_loop(0, qk_scr.shape[0] // TILE, turn, 0)
    head_from_line(3)
    wait_all(stores + [own_head] + head_partner)


def gather(x, wq, wk, wv, wo, devices, collective_id):
    rows, model_dim = x.shape
    f32 = jnp.float32
    head = (devices * rows, HEAD_SIZE)
    outs = (shape((devices, rows, model_dim), x.dtype), shape(head[::-1], f32), shape(head[::-1], f32), shape(head, x.dtype),
            shape((8,) + wo.shape, wo.dtype), shape((2 * HEAD_SIZE, model_dim), x.dtype), shape((HEAD_SIZE, model_dim), x.dtype))
    width = 3 * HEAD_SIZE
    scratch = [pltpu.VMEM((devices, rows, model_dim), x.dtype), pltpu.VMEM((model_dim, width), x.dtype),
               pltpu.VMEM((width, model_dim), x.dtype), pltpu.VMEM((devices * rows, 2 * HEAD_SIZE), f32), pltpu.VMEM((2 * rows, width), f32)]
    return call(gather_kernel, outs, (x, wq, wk, wv, wo), [ANY] * 5, (ANY, VMEM, VMEM, VMEM, ANY, ANY, ANY), scratch, collective_id, 62)


def nt(a, b):
    return lax.dot_general(a, b, (((1,), (1,)), ((), ())), preferred_element_type=jnp.float32)


def tn(a, b):
    return lax.dot_general(a, b, (((0,), (0,)), ((), ())), preferred_element_type=jnp.float32)


def nn(a, b):
    return lax.dot_general(a, b, (((1,), (0,)), ((), ())), preferred_element_type=jnp.float32)


def fold_rows(values, op):
    return op(values.reshape(values.shape[0] // 8, 8, values.shape[1]), axis=0)


def block_rows(j):
    return pl.ds(pl.multiple_of(j * BLOCK, BLOCK), BLOCK)


def diagonal_mask():
    keys = lax.broadcasted_iota(jnp.int32, (BLOCK, BLOCK), 0)
    queries = lax.broadcasted_iota(jnp.int32, (BLOCK, BLOCK), 1)
    return keys <= queries


def attention_kernel(q_ref, k_ref, v_ref, o_ref, ot_ref, max_ref, inv_ref, s_scr, acc_scr):
    i = pl.program_id(0)
    q_blk = q_ref[...]

    def score(j, top):
        s = tn(k_ref[:, block_rows(j)], q_blk) * (ATTN_SCALE * LOG2E)
        s_scr[block_rows(j), :] = s
        return jnp.maximum(top, fold_rows(s, jnp.max))

    s = jnp.where(diagonal_mask(), tn(k_ref[:, block_rows(i)], q_blk) * (ATTN_SCALE * LOG2E), -1e30)
    s_scr[block_rows(i), :] = s
    top = lax.fori_loop(0, i, score, fold_rows(s, jnp.max))
    top = jnp.max(top, axis=0, keepdims=True)

    def weigh(j, total):
        p = jnp.exp2(s_scr[block_rows(j), :] - top)
        s_scr[block_rows(j), :] = p
        return total + fold_rows(p, jnp.sum)

    total = lax.fori_loop(0, i + 1, weigh, jnp.zeros((8, BLOCK), jnp.float32))
    inv = 1.0 / jnp.sum(total, axis=0, keepdims=True)
    max_ref[...] = top
    inv_ref[...] = inv
    acc_scr[...] = jnp.zeros_like(acc_scr)

    def gather(j, carry):
        p = (s_scr[block_rows(j), :] * inv).astype(jnp.bfloat16)
        acc_scr[...] += tn(v_ref[block_rows(j), :], p)
        return carry

    lax.fori_loop(0, i + 1, gather, 0)
    o_ref[...] = acc_scr[...].T.astype(jnp.bfloat16)
    ot_ref[...] = acc_scr[...].astype(jnp.bfloat16)


def attention(q, k, v):
    seq_len = v.shape[0]
    steps = seq_len // BLOCK
    rows = pl.BlockSpec((BLOCK, HEAD_SIZE), lambda i: (i, 0))
    whole = pl.BlockSpec((seq_len, HEAD_SIZE), lambda i: (0, 0))
    line = pl.BlockSpec((1, BLOCK), lambda i: (0, i))
    columns = pl.BlockSpec((HEAD_SIZE, BLOCK), lambda i: (0, i))
    wide = pl.BlockSpec((HEAD_SIZE, seq_len), lambda i: (0, 0))
    return pl.pallas_call(
        attention_kernel,
        grid=(steps,),
        out_shape=(jax.ShapeDtypeStruct((seq_len, HEAD_SIZE), jnp.bfloat16),
                   jax.ShapeDtypeStruct((HEAD_SIZE, seq_len), jnp.bfloat16),
                   jax.ShapeDtypeStruct((1, seq_len), jnp.float32),
                   jax.ShapeDtypeStruct((1, seq_len), jnp.float32)),
        in_specs=[columns, wide, whole], out_specs=(rows, columns, line, line),
        scratch_shapes=[pltpu.VMEM((seq_len, BLOCK), jnp.float32), pltpu.VMEM((HEAD_SIZE, BLOCK), jnp.float32)],
        compiler_params=pltpu.CompilerParams(dimension_semantics=("arbitrary",), vmem_limit_bytes=40 << 20),
        cost_estimate=pl.CostEstimate(flops=8 * seq_len * seq_len * HEAD_SIZE, bytes_accessed=8 * seq_len * HEAD_SIZE, transcendentals=0),
    )(q, k, v)


def attention_grad_kernel(q_ref, k_ref, v_ref, do_ref, max_ref, inv_ref, dq_ref, dk_ref, dv_ref, dvt_ref, p_scr, dp_scr, dq_scr, dk_scr, dv_scr):
    i = pl.program_id(0)
    q_blk, do_blk = q_ref[...], do_ref[...]
    top, inv = max_ref[...], inv_ref[...]

    @pl.when(i == 0)
    def _():
        dk_scr[...] = jnp.zeros_like(dk_scr)
        dv_scr[...] = jnp.zeros_like(dv_scr)

    def scores(j, mask, delta):
        rows = block_rows(j)
        s = tn(k_ref[:, rows], q_blk) * (ATTN_SCALE * LOG2E)
        if mask is not None:
            s = jnp.where(mask, s, -1e30)
        p = jnp.exp2(s - top) * inv
        dp = nt(v_ref[rows, :], do_blk)
        p_scr[rows, :] = p
        dp_scr[rows, :] = dp
        dv_scr[rows, :] += nn(p.astype(jnp.bfloat16), do_blk)
        return delta + fold_rows(p * dp, jnp.sum)

    delta = scores(i, diagonal_mask(), jnp.zeros((8, BLOCK), jnp.float32))
    delta = lax.fori_loop(0, i, lambda j, d: scores(j, None, d), delta)
    delta = jnp.sum(delta, axis=0, keepdims=True)
    dq_scr[...] = jnp.zeros_like(dq_scr)

    def grads(j, carry):
        rows = block_rows(j)
        ds = (p_scr[rows, :] * (dp_scr[rows, :] - delta) * ATTN_SCALE).astype(jnp.bfloat16)
        dk_scr[:, rows] += nt(q_blk, ds)
        dq_scr[...] += nn(k_ref[:, rows], ds)
        return carry

    lax.fori_loop(0, i + 1, grads, 0)
    dq_ref[...] = dq_scr[...]

    @pl.when(i == pl.num_programs(0) - 1)
    def _():
        dk_ref[...] = dk_scr[...]
        dv_ref[...] = dv_scr[...].astype(jnp.bfloat16)

        def turn(j, carry):
            dvt_ref[:, block_rows(j)] = dv_scr[block_rows(j), :].T.astype(jnp.bfloat16)
            return carry

        lax.fori_loop(0, pl.num_programs(0), turn, 0)


def attention_grad(q, k, v, do, top, inv):
    seq_len = v.shape[0]
    steps = seq_len // BLOCK
    rows = pl.BlockSpec((BLOCK, HEAD_SIZE), lambda i: (i, 0))
    whole = pl.BlockSpec((seq_len, HEAD_SIZE), lambda i: (0, 0))
    line = pl.BlockSpec((1, BLOCK), lambda i: (0, i))
    columns = pl.BlockSpec((HEAD_SIZE, BLOCK), lambda i: (0, i))
    wide = pl.BlockSpec((HEAD_SIZE, seq_len), lambda i: (0, 0))
    full, turned = (seq_len, HEAD_SIZE), (HEAD_SIZE, seq_len)
    return pl.pallas_call(
        attention_grad_kernel,
        grid=(steps,),
        out_shape=(shape(turned, jnp.float32), shape(turned, jnp.float32), shape(full, jnp.bfloat16), shape(turned, jnp.bfloat16)),
        in_specs=[columns, wide, whole, rows, line, line], out_specs=(columns, wide, whole, wide),
        scratch_shapes=[pltpu.VMEM((seq_len, BLOCK), jnp.float32), pltpu.VMEM((seq_len, BLOCK), jnp.float32),
                        pltpu.VMEM((HEAD_SIZE, BLOCK), jnp.float32), pltpu.VMEM(turned, jnp.float32), pltpu.VMEM(full, jnp.float32)],
        compiler_params=pltpu.CompilerParams(dimension_semantics=("arbitrary",), vmem_limit_bytes=48 << 20),
        cost_estimate=pl.CostEstimate(flops=20 * seq_len * seq_len * HEAD_SIZE, bytes_accessed=20 * seq_len * HEAD_SIZE, transcendentals=0),
    )(q, k, v, do, top, inv)


COLUMN_GROUPS = [[z * 8 + c * 2 + core for z in range(4) for core in range(2)] for c in range(4)]
PLANE_GROUPS = [[z * 8 + p for p in range(8)] for z in range(4)]


def lane_rows(values):
    return values.reshape(-1, 128)


def local_block(x_loc, wq_loc, wk_loc, wv_loc, wo_loc, gq_loc, gk_loc, g_attn, dy_loc):
    x_loc, dy_loc = x_loc[0], dy_loc[0]
    rows, model_dim = x_loc.shape
    bf16, f32 = jnp.bfloat16, jnp.float32
    x_blocks, q_raw, k_raw, v_head, wo_blocks, wqk_rows, wv_rows = gather(x_loc, wq_loc, wk_loc, wv_loc, wo_loc, 32, 9)
    wo_col = wo_blocks.reshape(8 * HEAD_SIZE, model_dim)
    x_full = x_blocks.reshape(32 * rows, model_dim)
    seq_len = x_full.shape[0]
    wv_plane = lax.all_gather(wv_rows, 'tp', axis=0, tiled=True, axis_index_groups=PLANE_GROUPS)
    cos_t, sin_t = lax.optimization_barrier(rope_tables(seq_len))
    stats = jnp.concatenate([lane_rows(jnp.sum(q_raw * q_raw, axis=0)), lane_rows(jnp.sum(k_raw * k_raw, axis=0))])
    sq_sums = all_sum(stats, 1).reshape(2, seq_len)
    inv_rms = lax.rsqrt(sq_sums / model_dim + NORM_EPS)[:, None, :]
    q_unit = q_raw * inv_rms[0]
    k_unit = k_raw * inv_rms[1]
    gq_f, gk_f = gq_loc.astype(f32)[:, None], gk_loc.astype(f32)[:, None]
    q_rot = rotate(q_unit * gq_f, cos_t, sin_t).astype(bf16)
    k_rot = rotate(k_unit * gk_f, cos_t, sin_t).astype(bf16)
    o_head, o_rows, top, inv = attention(q_rot, k_rot, v_head)

    o_col = exchange(
        o_head.reshape(4, 4, 2, rows, HEAD_SIZE), (4, rows, 8 * HEAD_SIZE), column_peer, 8,
        lambda ref, d: ref.at[d // 8, :, d % 2],
        lambda ref, d: ref.at[:, :, part(member_of(d), HEAD_SIZE)], 2)
    a_part = nn(o_col.reshape(4 * rows, 8 * HEAD_SIZE), wo_col)
    attn_loc = ring_sum(a_part.reshape(4, rows, model_dim), 3)

    post_rms = lax.rsqrt(jnp.mean(attn_loc * attn_loc, axis=-1, keepdims=True) + NORM_EPS)
    normed = attn_loc * post_rms
    ga_f = g_attn.astype(f32)
    dy_f = dy_loc.astype(f32)
    y_loc = (x_loc.astype(f32) + normed * ga_f).astype(bf16)
    ga_part = jnp.sum(dy_f * normed, axis=0)
    g_normed = dy_f * ga_f
    d_attn = (post_rms * (g_normed - normed * jnp.mean(g_normed * normed, axis=-1, keepdims=True))).astype(bf16)

    d_ring, d_below, d_top, wqk_after = spread(d_attn, wqk_rows, 4)
    wqk_plane = lax.all_gather(wqk_after, 'tp', axis=0, tiled=True, axis_index_groups=PLANE_GROUPS)
    d_col = nt(d_ring.reshape(4 * rows, model_dim), wo_col).astype(bf16)
    d_head = exchange(
        d_col.reshape(4, rows, 8 * HEAD_SIZE), (4, 4, 2, rows, HEAD_SIZE), column_peer, 8,
        lambda ref, d: ref.at[:, :, part(member_of(d), HEAD_SIZE)],
        lambda ref, d: ref.at[d // 8, :, d % 2], 5).reshape(seq_len, HEAD_SIZE)

    dq_rot, dk_rot, d_value, d_value_rows = attention_grad(q_rot, k_rot, v_head, d_head, top, inv)
    dq_hat = rotate_back(dq_rot, cos_t, sin_t)
    dk_hat = rotate_back(dk_rot, cos_t, sin_t)
    grad_gq = jnp.sum(dq_hat * q_unit, axis=1)
    grad_gk = jnp.sum(dk_hat * k_unit, axis=1)
    dq_unit = dq_hat * gq_f
    dk_unit = dk_hat * gk_f
    sums = jnp.concatenate([lane_rows(jnp.sum(dq_unit * q_unit, axis=0)), lane_rows(jnp.sum(dk_unit * k_unit, axis=0)), lane_rows(ga_part)])
    sums = all_sum(sums, 6)
    dots_rows = 2 * seq_len // 128
    unit_dots = sums[:dots_rows].reshape(2, seq_len)[:, None, :] / model_dim
    grad_ga = sums[dots_rows:].reshape(model_dim)
    dq_raw = (inv_rms[0] * (dq_unit - q_unit * unit_dots[0])).astype(bf16)
    dk_raw = (inv_rms[1] * (dk_unit - k_unit * unit_dots[1])).astype(bf16)
    dqk_rows = jnp.concatenate([dq_raw, dk_raw], axis=0)
    d_qk = dqk_rows.T

    dqk_plane, dv_plane, d_far, d_low = plane_exchange(
        d_qk.reshape(4, 8, rows, 2 * HEAD_SIZE), d_value.reshape(4, 8, rows, HEAD_SIZE), d_below, d_attn, 7)
    grad_x, grad_wq, grad_wk, grad_wv, grad_wo = final(
        dqk_plane.reshape(4 * rows, 16 * HEAD_SIZE), dv_plane.reshape(4 * rows, 8 * HEAD_SIZE), wqk_plane, wv_plane,
        d_ring, d_below, d_top, d_low, d_far, dqk_rows, d_value_rows, o_rows, dy_loc, x_full, 8)
    return (y_loc[None], grad_x[None], grad_wq, grad_wk, grad_wv, grad_wo,
            grad_gq.astype(bf16), grad_gk.astype(bf16), grad_ga.astype(bf16))


def solution(mesh):
    act_spec = P(None, 'tp', None)
    col_spec = P(None, 'tp')
    row_spec = P('tp', None)
    vec_spec = P('tp')
    in_specs = (act_spec, col_spec, col_spec, col_spec, row_spec, vec_spec, vec_spec, P(), act_spec)
    out_specs = (act_spec, act_spec, col_spec, col_spec, col_spec, row_spec, vec_spec, vec_spec, P())
    return jax.shard_map(local_block, mesh=mesh, in_specs=in_specs, out_specs=out_specs, check_vma=False)
```
